32 devices in a mesh: dp: 2 (over x), row: 4 (over y, core), col: 4 (over z).
Axes of the slice: x: 2, y: 2, z: 4, core: 2. Of those that a mesh axis runs over, the one named last changes fastest.
Arguments:
- x_img: bfloat16 [4, 1024, 1536], P('dp', 'row', 'col'), may hold values from -3 to 3
- x_txt: bfloat16 [4, 128, 1536], P('dp', 'row', 'col'), may hold values from -3 to 3
- condition: bfloat16 [4, 1536], P('dp', 'row'), may hold values from -6 to 6
- w_qkv: bfloat16 [2, 1536, 3, 1536], P(None, 'row', None, 'col'), may hold values from -0.15625 to 0.15625
- b_qv: float32 [2, 2, 1536], P(None, None, 'col'), may hold values from -3 to 3
- w_out: bfloat16 [2, 1536, 1536], P(None, 'col', 'row'), may hold values from -0.625 to 0.625
- b_out: float32 [2, 1536], P(None, 'col'), may hold values from -3 to 3
- w_up: bfloat16 [2, 1536, 6144], P(None, 'row', 'col'), may hold values from -0.15625 to 0.15625
- b_up: float32 [2, 6144], P(None, 'col'), may hold values from -3 to 3
- w_down: bfloat16 [2, 6144, 1536], P(None, 'col', 'row'), may hold values from -0.078125 to 0.078125
- b_down: float32 [2, 1536], P(None, 'col'), may hold values from -3 to 3
- w_ada: bfloat16 [2, 1536, 6, 1536], P(None, 'row', None, 'col'), may hold values from -0.21875 to 0.21875
- b_ada: float32 [2, 6, 1536], P(None, None, 'col'), may hold values from -3 to 3
- cot_img: bfloat16 [4, 1024, 1536], P('dp', 'row', 'col'), may hold values from -6 to 6
- cot_txt: bfloat16 [4, 128, 1536], P('dp', 'row', 'col'), may hold values from -6 to 6
Outputs:
- out_img: bfloat16 [4, 1024, 1536], P('dp', 'row', 'col')
- out_txt: bfloat16 [4, 128, 1536], P('dp', 'row', 'col')
- dx_img: float32 [4, 1024, 1536], P('dp', 'row', 'col')
- dx_txt: float32 [4, 128, 1536], P('dp', 'row', 'col')
- d_condition: float32 [4, 1536], P('dp', 'row')
- d_w_qkv: float32 [2, 1536, 3, 1536], P(None, 'row', None, 'col')
- d_b_qv: float32 [2, 2, 1536], P(None, None, 'col')
- d_w_out: float32 [2, 1536, 1536], P(None, 'col', 'row')
- d_b_out: float32 [2, 1536], P(None, 'col')
- d_w_up: float32 [2, 1536, 6144], P(None, 'row', 'col')
- d_b_up: float32 [2, 6144], P(None, 'col')
- d_w_down: float32 [2, 6144, 1536], P(None, 'col', 'row')
- d_b_down: float32 [2, 1536], P(None, 'col')
- d_w_ada: float32 [2, 1536, 6, 1536], P(None, 'row', None, 'col')
- d_b_ada: float32 [2, 6, 1536], P(None, None, 'col')
The draws below stay inside these ranges and needn't reach their ends.
All inputs are finite; a program needn't handle non-finite values.
Results may differ from the reference program's by a relative error of at most 0.017.
The reference program's roundings to bfloat16 on the way count: a program that leaves them out, or rounds other values in their place, can miss the bound.
Values may be sent and summed in bfloat16 or wider, within the bound.
A program may use at most 192 MiB of HBM per device.

```python
from functools import partial
import jax
import jax.numpy as jnp
from jax import lax

D = 1536
H = 24
HD = 64
FF = 6144
DC = 1536
IMG = 1024
TXT = 128
SEQS = 4


def block_levels(rng, shape, cuts, smallest, largest):
    factor_of, own = 1.0, jax.random.fold_in(rng, 6)
    for axis_at, blocks in cuts:
        heights = jnp.exp(jax.random.uniform(jax.random.fold_in(own, axis_at), (blocks,), jnp.float32, smallest / len(cuts), largest / len(cuts)))
        factor_of = factor_of * jnp.repeat(heights, shape[axis_at] // blocks).reshape([-1 if axis == axis_at else 1 for axis in range(len(shape))])
    return factor_of


def noise(own_key, dims, scale, bound, cuts=(), held_as=jnp.bfloat16):
    drawn = jax.random.normal(own_key, dims, jnp.float32) * scale
    if len(cuts) > 0:
        drawn = block_levels(own_key, dims, cuts, -0.22, 0.18) * drawn
    return jnp.clip(drawn, min=-bound, max=bound).astype(held_as)


def setup_inputs(seed: int = 0) -> dict:
    streams_of = jax.random.split(jax.random.key(seed), 16)
    x_img = noise(streams_of[0], (SEQS, IMG, D), 0.5, 3.0, ((0, 2), (1, 4), (2, 4)))
    x_txt = noise(streams_of[1], (SEQS, TXT, D), 0.5, 3.0, ((0, 2), (1, 4), (2, 4)))
    condition = noise(streams_of[2], (SEQS, DC), 1.0, 6.0, ((0, 2), (1, 4)))
    w_qkv = noise(streams_of[3], (2, D, 3, D), D ** -0.5, 0.15625, ((1, 4), (3, 4)))
    b_qv = noise(streams_of[4], (2, 2, D), 0.5, 3.0, ((2, 4),), jnp.float32)
    w_out = noise(streams_of[5], (2, D, D), (D // 16) ** -0.5, 0.625, ((1, 4), (2, 4)))
    b_out = noise(streams_of[6], (2, D), 0.5, 3.0, ((1, 4),), jnp.float32)
    w_up = noise(streams_of[7], (2, D, FF), D ** -0.5, 0.15625, ((1, 4), (2, 4)))
    b_up = noise(streams_of[8], (2, FF), 0.5, 3.0, ((1, 4),), jnp.float32)
    w_down = noise(streams_of[9], (2, FF, D), FF ** -0.5, 0.078125, ((1, 4), (2, 4)))
    b_down = noise(streams_of[10], (2, D), 0.5, 3.0, ((1, 4),), jnp.float32)
    w_ada = noise(streams_of[11], (2, DC, 6, D), (DC // 2) ** -0.5, 0.21875, ((1, 4), (3, 4)))
    b_ada = noise(streams_of[12], (2, 6, D), 0.5, 3.0, ((2, 4),), jnp.float32)
    cot_img = noise(streams_of[13], (SEQS, IMG, D), 1.0, 6.0, ((0, 2), (1, 4), (2, 4)))
    cot_txt = noise(streams_of[14], (SEQS, TXT, D), 1.0, 6.0, ((0, 2), (1, 4), (2, 4)))
    return {"x_img": x_img, "x_txt": x_txt, "condition": condition, "w_qkv": w_qkv, "b_qv": b_qv, "w_out": w_out, "b_out": b_out, "w_up": w_up, "b_up": b_up, "w_down": w_down, "b_down": b_down, "w_ada": w_ada, "b_ada": b_ada, "cot_img": cot_img, "cot_txt": cot_txt}


EPSILON = 1e-06
GELU_ROOT = 0.7978845608028654
GELU_CUBIC = 0.044715

def gelu_pair(inputs):
    inner = GELU_ROOT * (inputs + GELU_CUBIC * inputs * inputs * inputs)
    tanh_value = jnp.tanh(inner)
    result = 0.5 * inputs * (1.0 + tanh_value)
    derivative = 0.5 * (1.0 + tanh_value) + 0.5 * inputs * (1.0 - tanh_value * tanh_value) * GELU_ROOT * (1.0 + 3.0 * GELU_CUBIC * inputs * inputs)
    return (result, derivative)

def layer_norm(values):
    centre_mean = lax.optimization_barrier(jnp.mean(values, axis=-1, keepdims=True))
    centred = values - centre_mean
    variance = lax.optimization_barrier(jnp.mean(centred * centred, axis=-1, keepdims=True))
    inverse = lax.rsqrt(variance + EPSILON)
    return (centred * inverse, inverse)

def norm_back(d_normed, normed, inverse):
    first_mean = lax.optimization_barrier(jnp.mean(d_normed, axis=-1, keepdims=True))
    second_mean = lax.optimization_barrier(jnp.mean(d_normed * normed, axis=-1, keepdims=True))
    return inverse * (d_normed - first_mean - normed * second_mean)

def attend_packed(packed, score_scale):
    queries, key_block, value_block = packed
    scores = jnp.dot(queries, key_block.T, preferred_element_type=jnp.float32) * score_scale
    highest = lax.optimization_barrier(jnp.max(scores, axis=-1, keepdims=True))
    log_total = highest + jnp.log(lax.optimization_barrier(jnp.sum(jnp.exp(scores - highest), axis=-1, keepdims=True)))
    soft_weights = jnp.exp(scores - log_total).astype(jnp.bfloat16)
    attended = jnp.dot(soft_weights, value_block, preferred_element_type=jnp.float32).astype(jnp.bfloat16)
    return (attended, log_total[:, 0])

def attend_back_packed(packed, score_scale):
    queries, key_block, value_block, attended, log_total, d_attended = packed
    scores = jnp.dot(queries, key_block.T, preferred_element_type=jnp.float32) * score_scale
    soft_weights = jnp.exp(scores - log_total[:, None])
    soft_bf = soft_weights.astype(jnp.bfloat16)
    d_values = jnp.dot(soft_bf.T, d_attended, preferred_element_type=jnp.float32).astype(jnp.bfloat16)
    d_soft = jnp.dot(d_attended, value_block.T, preferred_element_type=jnp.float32)
    centre = lax.optimization_barrier(jnp.sum(d_attended.astype(jnp.float32) * attended.astype(jnp.float32), axis=-1, keepdims=True))
    d_scores = (soft_weights * (d_soft - centre)).astype(jnp.bfloat16)
    d_queries = (jnp.dot(d_scores, key_block, preferred_element_type=jnp.float32) * score_scale).astype(jnp.bfloat16)
    d_keys = (jnp.dot(d_scores.T, queries, preferred_element_type=jnp.float32) * score_scale).astype(jnp.bfloat16)
    return (d_queries, d_keys, d_values)

def reference(x_img, x_txt, condition, w_qkv, b_qv, w_out, b_out, w_up, b_up, w_down, b_down, w_ada, b_ada, cot_img, cot_txt):
    score_scale = HD ** (-0.5)
    joint_len = IMG + TXT
    ada_flat = [w_ada[stream].reshape(DC, 6 * D) for stream in range(2)]
    ada_wide = [ada_flat[stream].astype(jnp.float32) for stream in range(2)]
    qkv_flat = [w_qkv[stream].reshape(D, 3 * D) for stream in range(2)]
    qkv_bias = [jnp.stack([b_qv[stream, 0], jnp.zeros((D,), jnp.float32), b_qv[stream, 1]], axis=0).reshape(3 * D) for stream in range(2)]

    def one_sequence(totals, inputs):
        seq_img, seq_txt, cond_row, cot_first, cot_second = inputs
        cond_wide = cond_row.astype(jnp.float32)
        cond_act = jax.nn.silu(cond_wide).astype(jnp.bfloat16)
        activations = (seq_img, seq_txt)
        cotangents = (cot_first, cot_second)
        kept = []
        qkv_parts = []
        for stream in range(2):
            mods = jnp.dot(cond_act[None, :], ada_flat[stream], preferred_element_type=jnp.float32).reshape(6, D) + b_ada[stream]
            resid = activations[stream].astype(jnp.float32)
            normed_one, inverse_one = layer_norm(resid)
            hidden_one = (normed_one * (1.0 + mods[1]) + mods[0]).astype(jnp.bfloat16)
            projected = (jnp.dot(hidden_one, qkv_flat[stream], preferred_element_type=jnp.float32) + qkv_bias[stream]).astype(jnp.bfloat16)
            kept.append((mods, resid, normed_one, inverse_one, hidden_one))
            qkv_parts.append(projected)
        joint = jnp.concatenate(qkv_parts, axis=0).reshape(joint_len, 3, H, HD)
        heads = jnp.transpose(joint, (1, 2, 0, 3))
        attended, log_total = lax.map(partial(attend_packed, score_scale=score_scale), (heads[0], heads[1], heads[2]))
        attn_rows = jnp.transpose(attended, (1, 0, 2)).reshape(joint_len, D)
        attn_parts = (attn_rows[:IMG], attn_rows[IMG:])
        later = []
        d_att_parts = []
        results = []
        for stream in range(2):
            mods, resid, normed_one, inverse_one, hidden_one = kept[stream]
            attn_in = attn_parts[stream]
            attn_branch = jnp.dot(attn_in, w_out[stream], preferred_element_type=jnp.float32) + b_out[stream]
            middle = resid + mods[2] * attn_branch
            normed_two, inverse_two = layer_norm(middle)
            hidden_two = (normed_two * (1.0 + mods[4]) + mods[3]).astype(jnp.bfloat16)
            pre_value = jnp.dot(hidden_two, w_up[stream], preferred_element_type=jnp.float32) + b_up[stream]
            gelu_value, gelu_slope = gelu_pair(pre_value)
            act_bf = gelu_value.astype(jnp.bfloat16)
            mlp_branch = jnp.dot(act_bf, w_down[stream], preferred_element_type=jnp.float32) + b_down[stream]
            results.append((middle + mods[5] * mlp_branch).astype(jnp.bfloat16))
            grad = cotangents[stream].astype(jnp.float32)
            d_mlp = grad * mods[5]
            d_mlp_bf = d_mlp.astype(jnp.bfloat16)
            d_pre = jnp.dot(d_mlp_bf, w_down[stream].T, preferred_element_type=jnp.float32) * gelu_slope
            d_pre_bf = d_pre.astype(jnp.bfloat16)
            d_hidden_two = jnp.dot(d_pre_bf, w_up[stream].T, preferred_element_type=jnp.float32)
            d_middle = grad + norm_back(d_hidden_two * (1.0 + mods[4]), normed_two, inverse_two)
            d_branch = d_middle * mods[2]
            d_branch_bf = d_branch.astype(jnp.bfloat16)
            d_att_parts.append(jnp.dot(d_branch_bf, w_out[stream].T, preferred_element_type=jnp.float32).astype(jnp.bfloat16))
            grad_down = jnp.dot(act_bf.T, d_mlp_bf, preferred_element_type=jnp.float32)
            grad_up = jnp.dot(hidden_two.T, d_pre_bf, preferred_element_type=jnp.float32)
            grad_out = jnp.dot(attn_in.T, d_branch_bf, preferred_element_type=jnp.float32)
            row_sums = [lax.optimization_barrier(jnp.sum(d_middle * attn_branch, axis=0)), lax.optimization_barrier(jnp.sum(d_hidden_two, axis=0)), lax.optimization_barrier(jnp.sum(d_hidden_two * normed_two, axis=0)), lax.optimization_barrier(jnp.sum(grad * mlp_branch, axis=0))]
            later.append((d_middle, grad_down, lax.optimization_barrier(jnp.sum(d_mlp, axis=0)), grad_up, lax.optimization_barrier(jnp.sum(d_pre, axis=0)), grad_out, lax.optimization_barrier(jnp.sum(d_branch, axis=0)), row_sums))
        d_joint = jnp.concatenate(d_att_parts, axis=0).reshape(joint_len, H, HD)
        d_heads = jnp.transpose(d_joint, (1, 0, 2))
        d_queries, d_keys, d_values = lax.map(partial(attend_back_packed, score_scale=score_scale), (heads[0], heads[1], heads[2], attended, log_total, d_heads))
        d_qkv_rows = jnp.stack([jnp.transpose(d_queries, (1, 0, 2)).reshape(joint_len, D), jnp.transpose(d_keys, (1, 0, 2)).reshape(joint_len, D), jnp.transpose(d_values, (1, 0, 2)).reshape(joint_len, D)], axis=1)
        d_qkv_parts = (d_qkv_rows[:IMG].reshape(IMG, 3 * D), d_qkv_rows[IMG:].reshape(TXT, 3 * D))
        increments = [[], [], [], [], [], [], [], [], [], []]
        d_inputs = []
        d_silu = jnp.zeros((DC,), jnp.float32)
        for stream in range(2):
            mods, resid, normed_one, inverse_one, hidden_one = kept[stream]
            d_middle, grad_down, bias_down, grad_up, bias_up, grad_out, bias_out, row_sums = later[stream]
            d_qkv = d_qkv_parts[stream]
            d_qkv_wide = d_qkv.astype(jnp.float32)
            grad_qkv = jnp.dot(hidden_one.T, d_qkv, preferred_element_type=jnp.float32)
            bias_qv = jnp.stack([lax.optimization_barrier(jnp.sum(d_qkv_wide[:, :D], axis=0)), lax.optimization_barrier(jnp.sum(d_qkv_wide[:, 2 * D:], axis=0))], axis=0)
            d_hidden_one = jnp.dot(d_qkv, qkv_flat[stream].T, preferred_element_type=jnp.float32)
            d_inputs.append(d_middle + norm_back(d_hidden_one * (1.0 + mods[1]), normed_one, inverse_one))
            d_mods = jnp.stack([lax.optimization_barrier(jnp.sum(d_hidden_one, axis=0)), lax.optimization_barrier(jnp.sum(d_hidden_one * normed_one, axis=0)), row_sums[0], row_sums[1], row_sums[2], row_sums[3]], axis=0)
            d_mods_flat = d_mods.reshape(6 * D)
            grad_ada = cond_act.astype(jnp.float32)[:, None] * d_mods_flat[None, :]
            d_silu = d_silu + jnp.dot(ada_wide[stream], d_mods_flat, precision=lax.Precision.HIGHEST)
            for position, value_item in enumerate((grad_qkv, bias_qv, grad_out, bias_out, grad_up, bias_up, grad_down, bias_down, grad_ada, d_mods)):
                increments[position].append(value_item)
        new_totals = tuple((totals[position] + jnp.stack(increments[position], axis=0) for position in range(10)))
        sigmoid_cond = jax.nn.sigmoid(cond_wide)
        d_cond = d_silu * sigmoid_cond * (1.0 + cond_wide * (1.0 - sigmoid_cond))
        return (new_totals, (results[0], results[1], d_inputs[0], d_inputs[1], d_cond))
    zero_totals = (jnp.zeros((2, D, 3 * D), jnp.float32), jnp.zeros((2, 2, D), jnp.float32), jnp.zeros((2, D, D), jnp.float32), jnp.zeros((2, D), jnp.float32), jnp.zeros((2, D, FF), jnp.float32), jnp.zeros((2, FF), jnp.float32), jnp.zeros((2, FF, D), jnp.float32), jnp.zeros((2, D), jnp.float32), jnp.zeros((2, DC, 6 * D), jnp.float32), jnp.zeros((2, 6, D), jnp.float32))
    totals, per_seq = lax.scan(one_sequence, zero_totals, (x_img, x_txt, condition, cot_img, cot_txt))
    out_img, out_txt, dx_img, dx_txt, d_condition = per_seq
    return (out_img, out_txt, dx_img, dx_txt, d_condition, totals[0].reshape(2, D, 3, D), totals[1], totals[2], totals[3], totals[4], totals[5], totals[6], totals[7], totals[8].reshape(2, DC, 6, D), totals[9])
```

```python
from functools import partial

import jax
import jax.numpy as jnp
from jax import lax
from jax.experimental import pallas as pl
from jax.experimental.pallas import tpu as pltpu
from jax.sharding import PartitionSpec as P

HD = 64
EPSILON = 1e-06
GELU_ROOT = 0.7978845608028654
GELU_CUBIC = 0.044715
BF = jnp.bfloat16
F32 = jnp.float32
MESH = pl.DeviceIdType.MESH
ANY = pl.BlockSpec(memory_space=pl.ANY)
VM = pl.BlockSpec(memory_space=pltpu.VMEM)
VMEM_LIMIT = 60 * 1024 * 1024


def struct(shape, dtype):
    return jax.ShapeDtypeStruct(shape, dtype)


def aligned(index, size):
    return pl.ds(pl.multiple_of(index * size, size), size)


def send(src, dst, send_sem, recv_sem, axis, index):
    return pltpu.make_async_remote_copy(
        src_ref=src,
        dst_ref=dst,
        send_sem=send_sem,
        recv_sem=recv_sem,
        device_id={axis: index},
        device_id_type=MESH,
    )


def flip(index):
    return index + 1 - 2 * lax.rem(index, 2)


def flip_far(index):
    return lax.rem(index + 2, 4)


def greet(pairs):
    barrier = pltpu.get_barrier_semaphore()
    for axis, index in pairs:
        pl.semaphore_signal(barrier, inc=1, device_id={axis: index}, device_id_type=MESH)
    pl.semaphore_wait(barrier, len(pairs))


def others(axis, count):
    me = lax.axis_index(axis)
    return [(axis, lax.rem(me + step, count)) for step in range(1, count)]


class LineGather:
    def __init__(self, view, count, place, send_sems, recv_sems):
        self.view, self.count, self.place = view, count, place
        self.send_sems, self.recv_sems = send_sems, recv_sems

    def copy(self, side, step, arriving):
        place = self.place
        if side == 0:
            block = place - step - (1 if arriving else 0)
            peer = place + 1
        else:
            block = place + step + (1 if arriving else 0)
            peer = place - 1
        view = self.view(block)
        return send(
            view, view, self.send_sems.at[side, step], self.recv_sems.at[side, step], "col", peer
        )

    def sends(self, side, step):
        if side == 0:
            return jnp.logical_and(self.place - step >= 0, self.place < self.count - 1)
        return jnp.logical_and(self.place + step <= self.count - 1, self.place > 0)

    def arrives(self, side, step):
        if side == 0:
            return self.place - 1 - step >= 0
        return self.place + 1 + step <= self.count - 1

    def start(self, step):
        for side in range(2):

            @pl.when(self.sends(side, step))
            def _():
                self.copy(side, step, False).start()

    def arrive(self, step):
        for side in range(2):

            @pl.when(self.arrives(side, step))
            def _():
                self.copy(side, step, True).wait_recv()

    def finish(self):
        for step in range(self.count - 1):
            for side in range(2):

                @pl.when(self.sends(side, step))
                def _():
                    self.copy(side, step, False).wait_send()


class LineReduce:
    def __init__(self, load, count, place, out_bufs, in_bufs, send_sems, recv_sems):
        self.load, self.count, self.place = load, count, place
        self.out_bufs, self.in_bufs = out_bufs, in_bufs
        self.send_sems, self.recv_sems = send_sems, recv_sems

    def copy(self, side, slot):
        peer = self.place + 1 if side == 0 else self.place - 1
        return send(
            self.out_bufs.at[side, slot],
            self.in_bufs.at[side, slot],
            self.send_sems.at[side, slot],
            self.recv_sems.at[side, slot],
            "col",
            peer,
        )

    def has_behind(self, side):
        return self.place > 0 if side == 0 else self.place < self.count - 1

    def target(self, side, slot):
        return self.place + 1 + slot if side == 0 else self.place - 1 - slot

    def sends(self, side, slot):
        target = self.target(side, slot)
        return target <= self.count - 1 if side == 0 else target >= 0

    def step(self, number):
        slot = self.count - 2 - number
        for side in range(2):

            @pl.when(self.sends(side, slot))
            def _():
                target = self.target(side, slot)
                if slot < self.count - 2:

                    @pl.when(self.has_behind(side))
                    def _():
                        self.copy(side, slot + 1).wait_recv()
                        self.out_bufs[side, slot] = (
                            self.load(target).astype(F32) + self.in_bufs[side, slot + 1].astype(F32)
                        ).astype(BF)

                    @pl.when(jnp.logical_not(self.has_behind(side)))
                    def _():
                        self.out_bufs[side, slot] = self.load(target)

                else:
                    self.out_bufs[side, slot] = self.load(target)
                self.copy(side, slot).start()

    def total(self, store):
        own = self.load(self.place).astype(F32)

        @pl.when(self.place == 0)
        def _():
            self.copy(1, 0).wait_recv()
            store(own + self.in_bufs[1, 0].astype(F32))

        @pl.when(self.place == self.count - 1)
        def _():
            self.copy(0, 0).wait_recv()
            store(own + self.in_bufs[0, 0].astype(F32))

        @pl.when(jnp.logical_and(self.place > 0, self.place < self.count - 1))
        def _():
            self.copy(0, 0).wait_recv()
            self.copy(1, 0).wait_recv()
            store(own + self.in_bufs[0, 0].astype(F32) + self.in_bufs[1, 0].astype(F32))

    def finish(self):
        for slot in range(self.count - 1):
            for side in range(2):

                @pl.when(self.sends(side, slot))
                def _():
                    self.copy(side, slot).wait_send()


def communicate(kernel, name, collective_id, **kwargs):
    return pl.pallas_call(
        kernel,
        name=name,
        compiler_params=pltpu.CompilerParams(
            collective_id=collective_id, has_side_effects=True, vmem_limit_bytes=VMEM_LIMIT
        ),
        **kwargs,
    )


class WeightFlow:
    def __init__(self, kinds, shards, fulls, subs, send_sems, recv_sems):
        self.kinds, self.shards, self.fulls, self.subs = kinds, shards, fulls, subs
        self.send_sems, self.recv_sems = send_sems, recv_sems
        self.pieces = [(n, s, u) for n in range(len(kinds)) for s in range(2) for u in range(subs)]
        self.row = lax.axis_index("row")
        self.half = lax.rem(lax.axis_index("dp"), 2)
        self.mate = flip(lax.axis_index("dp"))
        self.sib, self.far = flip(self.row), flip_far(self.row)

    @staticmethod
    def sem_shape(count, subs):
        return (count * 2 * subs, 5)

    def split(self, depth, sub, part):
        if part is None:
            size = depth // self.subs
            return pl.ds(sub * size, size)
        size = depth // (2 * self.subs)
        return aligned(2 * sub + part, size)

    def view(self, piece, block, part):
        number, stream, sub = self.pieces[piece]
        kind, ref, shard = self.kinds[number], self.fulls[number], self.shards[number]
        if kind == "qkv" or kind == "up":
            depth = shard.shape[-2]
            if part is None:
                size = depth // self.subs
                rows = aligned(block * self.subs + sub, size)
            else:
                rows = aligned(block * 2 * self.subs + 2 * sub + part, depth // (2 * self.subs))
            return ref.at[stream, :, rows, :] if kind == "qkv" else ref.at[stream, rows, :]
        return ref.at[stream, self.split(shard.shape[1], sub, part), aligned(block, shard.shape[2])]

    def source(self, piece, part):
        number, stream, sub = self.pieces[piece]
        ref = self.shards[number]
        rows = self.split(ref.shape[-2], sub, part)
        return ref.at[stream, :, rows, :] if self.kinds[number] == "qkv" else ref.at[stream, rows, :]

    def copy(self, piece, kind):
        sems = (self.send_sems.at[piece, kind], self.recv_sems.at[piece, kind])
        if kind == 0:
            return send(self.source(piece, None), self.view(piece, self.row, None), *sems, "row", self.sib)
        if kind == 1:
            return send(self.source(piece, self.half), self.view(piece, self.row, self.half), *sems, "row", self.far)
        at = self.view(piece, self.far, 1 - self.half if kind == 4 else self.half)
        if kind == 2:
            return send(at, at, *sems, "dp", self.mate)
        return send(at, at, *sems, "row", self.sib)

    def land(self, piece, kind):
        if kind == 0:
            at = self.view(piece, self.sib, None)
        elif kind == 1:
            at = self.view(piece, self.far, self.half)
        elif kind == 2:
            at = self.view(piece, self.far, 1 - self.half)
        elif kind == 3:
            at = self.view(piece, flip(self.far), self.half)
        else:
            at = self.view(piece, flip(self.far), 1 - self.half)
        send(at, at, self.send_sems.at[piece, kind], self.recv_sems.at[piece, kind], "row", self.sib).wait_recv()

    def start(self, kind):
        for piece in range(len(self.pieces)):
            self.copy(piece, kind).start()

    def relay_y(self, piece):
        self.land(piece, 1)
        self.copy(piece, 2).start()
        self.copy(piece, 3).start()

    def relay_x(self, piece):
        self.land(piece, 2)
        self.copy(piece, 4).start()

    def finish(self):
        for piece in range(len(self.pieces)):
            for kind in (0, 3, 4):
                self.land(piece, kind)
        for piece in range(len(self.pieces)):
            for kind in range(5):
                self.copy(piece, kind).wait_send()

    def own_view(self, number):
        kind, ref, shard = self.kinds[number], self.fulls[number], self.shards[number]
        if kind == "qkv":
            return ref.at[:, :, aligned(self.row, shard.shape[2]), :]
        if kind == "up":
            return ref.at[:, aligned(self.row, shard.shape[1]), :]
        return ref.at[:, :, aligned(self.row, shard.shape[2])]


def gathered_shape(kind, shape):
    if kind == "qkv":
        return shape[:2] + (shape[2] * 4, shape[3])
    if kind == "up":
        return (shape[0], shape[1] * 4, shape[2])
    return shape[:2] + (shape[2] * 4,)


class OwnCopy:
    def __init__(self, src, stage, dst, sem_in, sem_out):
        self.first = pltpu.make_async_copy(src, stage, sem_in)
        self.second = pltpu.make_async_copy(stage, dst, sem_out)

    def begin(self):
        self.first.start()

    def settle(self):
        self.first.wait()
        self.second.start()

    def finish(self):
        self.second.wait()


def line_from(shard, full, width, cols, place, zs, zr):
    def at(block):
        return full.at[:, :, aligned(block, width)]

    line = LineGather(at, cols, place, zs, zr)

    def first():
        for side in range(2):
            peer = place + 1 if side == 0 else place - 1

            @pl.when(line.sends(side, 0))
            def _():
                send(shard, at(place), zs.at[side, 0], zr.at[side, 0], "col", peer).start()

    return line, first, at(place)


def prologue(cols, x_img, x_txt, qkv, out, table, bias):
    shards = (x_img, x_txt, qkv, out)
    width = x_img.shape[2]
    rows = 4
    kinds = ("qkv", "out")
    full_shapes = [s.shape[:2] + (s.shape[2] * cols,) for s in shards[:2]]
    full_shapes += [gathered_shape(k, s.shape) for k, s in zip(kinds, shards[2:])]
    table_shape = table.shape

    def kernel(*refs):
        shard = refs[:4]
        table_ref, bias_ref = refs[4:6]
        full = refs[6:10]
        mods_ref = refs[10]
        stage = refs[11:15]
        parts = refs[15]
        local_in, local_out, zs, zr, ws, wr, ms, mr = refs[16:]
        place = lax.axis_index("col")
        row = lax.axis_index("row")
        flow = WeightFlow(kinds, shard[2:], full[2:], 1, ws, wr)
        lines = [line_from(shard[n], full[n], width, cols, place, zs.at[n], zr.at[n]) for n in range(2)]
        owns = [OwnCopy(shard[n], stage[n], lines[n][2], local_in.at[n], local_out.at[n]) for n in range(2)]
        owns += [
            OwnCopy(shard[2 + n], stage[2 + n], flow.own_view(n), local_in.at[2 + n], local_out.at[2 + n])
            for n in range(2)
        ]
        for own in owns:
            own.begin()
        greet(others("row", rows) + others("col", cols) + [("dp", flow.mate)])

        def part_copy(step):
            return send(
                table_ref, parts.at[step - 1], ms.at[step - 1], mr.at[step - 1], "row", lax.rem(row + step, rows)
            )

        for step in range(1, rows):
            part_copy(step).start()
        for _, first, _ in lines:
            first()
        flow.start(1)
        flow.start(0)
        for step in range(1, rows):
            part_copy(step).wait()
        total = bias_ref[...]
        for index in range(rows):
            gap = lax.rem(row - index + rows, rows)
            theirs = parts[jnp.maximum(gap - 1, 0)]
            total = total + jnp.where(gap == 0, table_ref[...], theirs)
        mods_ref[place] = total

        def mod_copy(step):
            return send(
                mods_ref.at[place],
                mods_ref.at[place],
                ms.at[rows - 2 + step],
                mr.at[rows - 2 + step],
                "col",
                lax.rem(place + step, cols),
            )

        for step in range(1, cols):
            mod_copy(step).start()
        for own in owns:
            own.settle()
        flow.relay_y(0)
        for line, _, _ in lines:
            line.arrive(0)
            line.start(1)
        flow.relay_y(1)
        flow.relay_x(0)
        for step in range(2, cols - 1):
            for line, _, _ in lines:
                line.arrive(step - 1)
                line.start(step)
        flow.relay_y(2)
        flow.relay_x(1)
        flow.relay_y(3)
        flow.relay_x(2)
        flow.relay_x(3)
        for line, _, _ in lines:
            line.arrive(cols - 2)
        for step in range(1, cols):
            source_place = lax.rem(place - step + cols, cols)
            at = mods_ref.at[source_place]
            send(at, at, ms.at[rows - 2 + step], mr.at[rows - 2 + step], "col", source_place).wait_recv()
            mod_copy(step).wait_send()
        for line, _, _ in lines:
            line.finish()
        flow.finish()
        for own in owns:
            own.finish()

    return communicate(
        kernel,
        "prologue",
        0,
        out_shape=[struct(s, BF) for s in full_shapes] + [struct((cols,) + table_shape, F32)],
        in_specs=[ANY] * 4 + [VM, VM],
        out_specs=[ANY] * 4 + [VM],
        scratch_shapes=[pltpu.VMEM(s.shape, BF) for s in shards]
        + [
            pltpu.VMEM((rows - 1,) + table_shape, F32),
            pltpu.SemaphoreType.DMA((4,)),
            pltpu.SemaphoreType.DMA((4,)),
            pltpu.SemaphoreType.DMA((2, 2, cols - 1)),
            pltpu.SemaphoreType.DMA((2, 2, cols - 1)),
            pltpu.SemaphoreType.DMA(WeightFlow.sem_shape(2, 1)),
            pltpu.SemaphoreType.DMA(WeightFlow.sem_shape(2, 1)),
            pltpu.SemaphoreType.DMA((rows + cols - 2,)),
            pltpu.SemaphoreType.DMA((rows + cols - 2,)),
        ],
    )(*shards, table, bias)


def gather_keys(cols, kv_img, kv_txt, cot_img, cot_txt):
    two, seqs, img, width = kv_img.shape
    txt = kv_txt.shape[2]
    cots = (cot_img, cot_txt)

    def kernel(*refs):
        img_ref, txt_ref = refs[:2]
        cot_refs = refs[2:4]
        all_ref = refs[4]
        cot_full = refs[5:7]
        stage_img, stage_txt = refs[7:9]
        stage_cot = refs[9:11]
        local, ss, rs, zs, zr = refs[11:]
        row = lax.axis_index("row")
        place = lax.axis_index("col")
        sib, far = flip(row), flip_far(row)
        ins = [
            pltpu.make_async_copy(img_ref, stage_img, local.at[0]),
            pltpu.make_async_copy(txt_ref, stage_txt, local.at[1]),
        ]
        for copy in ins:
            copy.start()
        lines = [line_from(cot_refs[n], cot_full[n], width, cols, place, zs.at[n], zr.at[n]) for n in range(2)]
        owns = [
            OwnCopy(cot_refs[n], stage_cot[n], lines[n][2], local.at[6 + n], local.at[8 + n]) for n in range(2)
        ]
        for own in owns:
            own.begin()

        def img_at(block, index):
            return all_ref.at[block, index, :, pl.ds(0, img), :]

        def txt_at(block, index):
            return all_ref.at[block, index, :, pl.ds(img, txt), :]

        greet(others("row", 4) + others("col", cols))

        def direct(kind, index):
            peer = far if kind == 0 else sib
            return [
                send(img_ref.at[index], img_at(row, index), ss.at[kind, index, 0], rs.at[kind, index, 0], "row", peer),
                send(txt_ref.at[index], txt_at(row, index), ss.at[kind, index, 1], rs.at[kind, index, 1], "row", peer),
            ]

        def onward(index, block):
            return [
                send(img_at(block, index), img_at(block, index), ss.at[2, index, 0], rs.at[2, index, 0], "row", sib),
                send(txt_at(block, index), txt_at(block, index), ss.at[2, index, 1], rs.at[2, index, 1], "row", sib),
            ]

        def land(kind, index, block):
            for number, at in ((0, img_at(block, index)), (1, txt_at(block, index))):
                send(at, at, ss.at[kind, index, number], rs.at[kind, index, number], "row", sib).wait_recv()

        for kind in range(2):
            for index in range(2):
                for copy in direct(kind, index):
                    copy.start()
        for _, first, _ in lines:
            first()
        for copy in ins:
            copy.wait()
        outs = []
        for index in range(2):
            outs.append(pltpu.make_async_copy(stage_img.at[index], img_at(row, index), local.at[2 + index]))
            outs.append(pltpu.make_async_copy(stage_txt.at[index], txt_at(row, index), local.at[4 + index]))
        for copy in outs:
            copy.start()
        for own in owns:
            own.settle()
        land(0, 0, far)
        for copy in onward(0, far):
            copy.start()
        for line, _, _ in lines:
            line.arrive(0)
            line.start(1)
        land(0, 1, far)
        for copy in onward(1, far):
            copy.start()
        for step in range(2, cols - 1):
            for line, _, _ in lines:
                line.arrive(step - 1)
                line.start(step)
        for index in range(2):
            land(1, index, sib)
            land(2, index, flip(far))
        for line, _, _ in lines:
            line.arrive(cols - 2)
        for line, _, _ in lines:
            line.finish()
        for index in range(2):
            for kind in range(2):
                for copy in direct(kind, index):
                    copy.wait_send()
            for copy in onward(index, far):
                copy.wait_send()
        for copy in outs:
            copy.wait()
        for own in owns:
            own.finish()

    return communicate(
        kernel,
        "gather_keys",
        1,
        out_shape=[struct((4, two, seqs, img + txt, width), BF)]
        + [struct(c.shape[:2] + (width * cols,), BF) for c in cots],
        in_specs=[ANY] * 4,
        out_specs=[ANY] * 3,
        scratch_shapes=[
            pltpu.VMEM(kv_img.shape, BF),
            pltpu.VMEM(kv_txt.shape, BF),
            pltpu.VMEM(cot_img.shape, BF),
            pltpu.VMEM(cot_txt.shape, BF),
            pltpu.SemaphoreType.DMA((10,)),
            pltpu.SemaphoreType.DMA((3, 2, 2)),
            pltpu.SemaphoreType.DMA((3, 2, 2)),
            pltpu.SemaphoreType.DMA((2, 2, cols - 1)),
            pltpu.SemaphoreType.DMA((2, 2, cols - 1)),
        ],
    )(kv_img, kv_txt, cot_img, cot_txt)


def attend(q_img, q_txt, keys):
    seqs, img, width = q_img.shape
    txt = q_txt.shape[1]
    tokens = img + txt
    blocks = keys.shape[0]
    pairs = width // (2 * HD)
    scale = HD ** (-0.5)

    def kernel(qi_ref, qt_ref, k_ref, v_ref, oi_ref, ot_ref, lse_ref):
        queries = jnp.concatenate([qi_ref[...], qt_ref[...]], axis=0)
        key_block = k_ref[...].reshape(blocks * tokens, 2 * HD)
        value_block = v_ref[...].reshape(blocks * tokens, 2 * HD)
        low = lax.broadcasted_iota(jnp.int32, (tokens, 2 * HD), 1) < HD
        results, sums = [], []
        for head in range(2):
            mine = low if head == 0 else jnp.logical_not(low)
            chosen = jnp.where(mine, queries, jnp.zeros_like(queries))
            scores = (
                lax.dot_general(
                    chosen, key_block, (((1,), (1,)), ((), ())), preferred_element_type=F32
                )
                * scale
            )
            highest = jnp.max(scores, axis=-1, keepdims=True)
            grown = jnp.exp(scores - highest)
            total = jnp.sum(grown, axis=-1, keepdims=True)
            weights = (grown * (1.0 / total)).astype(BF)
            results.append(jnp.dot(weights, value_block, preferred_element_type=F32))
            sums.append(jnp.broadcast_to(highest + jnp.log(total), (tokens, 2 * HD)))
        attended = jnp.where(low, results[0], results[1]).astype(BF)
        oi_ref[...] = attended[:img]
        ot_ref[...] = attended[img:]
        lse_ref[...] = jnp.where(low, sums[0], sums[1])

    lanes = 2 * HD
    q_img_spec = pl.BlockSpec((None, img, lanes), lambda s, h: (s, 0, h))
    q_txt_spec = pl.BlockSpec((None, txt, lanes), lambda s, h: (s, 0, h))
    return pl.pallas_call(
        kernel,
        name="attend",
        grid=(seqs, pairs),
        in_specs=[
            q_img_spec,
            q_txt_spec,
            pl.BlockSpec((blocks, None, None, tokens, lanes), lambda s, h: (0, 0, s, 0, h)),
            pl.BlockSpec((blocks, None, None, tokens, lanes), lambda s, h: (0, 1, s, 0, h)),
        ],
        out_specs=[
            q_img_spec,
            q_txt_spec,
            pl.BlockSpec((None, None, tokens, lanes), lambda s, h: (s, h, 0, 0)),
        ],
        out_shape=[
            struct(q_img.shape, BF),
            struct(q_txt.shape, BF),
            struct((seqs, pairs, tokens, lanes), F32),
        ],
        compiler_params=pltpu.CompilerParams(vmem_limit_bytes=VMEM_LIMIT),
    )(q_img, q_txt, keys, keys)


def attend_back(q_img, q_txt, keys, o_img, o_txt, do_img, do_txt, lse):
    seqs, img, width = q_img.shape
    txt = q_txt.shape[1]
    tokens = img + txt
    blocks = keys.shape[0]
    pairs = width // (2 * HD)
    lanes = 2 * HD
    scale = HD ** (-0.5)
    over_last = (((1,), (1,)), ((), ()))
    over_first = (((0,), (0,)), ((), ()))

    def kernel(qi, qt, k_ref, v_ref, oi, ot, di, dt, lse_ref, dqi, dqt, dk_ref, dv_ref):
        queries = jnp.concatenate([qi[...], qt[...]], axis=0)
        attended = jnp.concatenate([oi[...], ot[...]], axis=0)
        d_attended = jnp.concatenate([di[...], dt[...]], axis=0)
        key_block = k_ref[...].reshape(blocks * tokens, lanes)
        value_block = v_ref[...].reshape(blocks * tokens, lanes)
        low = lax.broadcasted_iota(jnp.int32, (tokens, lanes), 1) < HD
        product = d_attended.astype(F32) * attended.astype(F32)
        d_q = []
        d_k = jnp.zeros((blocks * tokens, lanes), F32)
        d_v = jnp.zeros((blocks * tokens, lanes), F32)
        for head in range(2):
            mine = low if head == 0 else jnp.logical_not(low)
            zero = jnp.zeros_like(queries)
            q_head = jnp.where(mine, queries, zero)
            d_head = jnp.where(mine, d_attended, zero)
            centre = jnp.sum(jnp.where(mine, product, 0.0), axis=-1, keepdims=True)
            log_total = lse_ref[:, head * HD : head * HD + 1]
            scores = (
                lax.dot_general(q_head, key_block, over_last, preferred_element_type=F32) * scale
            )
            weights = jnp.exp(scores - log_total)
            d_weights = lax.dot_general(d_head, value_block, over_last, preferred_element_type=F32)
            d_scores = (weights * (d_weights - centre)).astype(BF)
            d_v = d_v + lax.dot_general(
                weights.astype(BF), d_head, over_first, preferred_element_type=F32
            )
            d_k = d_k + lax.dot_general(d_scores, q_head, over_first, preferred_element_type=F32)
            d_q.append(jnp.dot(d_scores, key_block, preferred_element_type=F32))
        d_queries = (jnp.where(low, d_q[0], d_q[1]) * scale).astype(BF)
        dqi[...] = d_queries[:img]
        dqt[...] = d_queries[img:]
        dk_ref[...] = (d_k * scale).astype(BF).reshape(blocks, tokens, lanes)
        dv_ref[...] = d_v.astype(BF).reshape(blocks, tokens, lanes)

    img_spec = pl.BlockSpec((None, img, lanes), lambda s, h: (s, 0, h))
    txt_spec = pl.BlockSpec((None, txt, lanes), lambda s, h: (s, 0, h))
    sums = pl.BlockSpec((blocks, None, tokens, lanes), lambda s, h: (0, s, 0, h))
    return pl.pallas_call(
        kernel,
        name="attend_back",
        grid=(seqs, pairs),
        in_specs=[
            img_spec,
            txt_spec,
            pl.BlockSpec((blocks, None, None, tokens, lanes), lambda s, h: (0, 0, s, 0, h)),
            pl.BlockSpec((blocks, None, None, tokens, lanes), lambda s, h: (0, 1, s, 0, h)),
            img_spec,
            txt_spec,
            img_spec,
            txt_spec,
            pl.BlockSpec((None, None, tokens, lanes), lambda s, h: (s, h, 0, 0)),
        ],
        out_specs=[img_spec, txt_spec, sums, sums],
        out_shape=[
            struct(q_img.shape, BF),
            struct(q_txt.shape, BF),
            struct((blocks, seqs, tokens, width), BF),
            struct((blocks, seqs, tokens, width), BF),
        ],
        compiler_params=pltpu.CompilerParams(vmem_limit_bytes=VMEM_LIMIT),
    )(q_img, q_txt, keys, keys, o_img, o_txt, do_img, do_txt, lse)


OVER_FIRST = (((0,), (0,)), ((), ()))
OVER_LAST = (((1,), (1,)), ((), ()))


def chunk_rows(img, txt, size):
    spans = [(1, 0, txt)]
    for first in range(0, img, size):
        spans.append((0, first, min(size, img - first)))
    return spans


def line_buffers(spans, slots, width):
    bufs = []
    for _, _, size in spans:
        bufs += [pltpu.VMEM((2, slots, size, width), BF)] * 2
    return bufs


def line_reduces(spans, parts, cols, place, width, bufs, ss, rs):
    reduces = []
    for number, (which, first, size) in enumerate(spans):
        src = parts[which]

        def load(block, src=src, first=first, size=size):
            return src[pl.ds(first, size), aligned(block, width)]

        reduces.append(
            LineReduce(load, cols, place, bufs[2 * number], bufs[2 * number + 1], ss.at[number], rs.at[number])
        )
    return reduces


def line_gathers(spans, outs, cols, place, width, ss, rs):
    gathers = []
    for number, (which, first, size) in enumerate(spans):
        dst = outs[which]

        def at(block, dst=dst, first=first, size=size):
            return dst.at[pl.ds(first, size), aligned(block, width)]

        gathers.append(LineGather(at, cols, place, ss.at[number], rs.at[number]))
    return gathers


class LineSum:
    def __init__(self, spans, parts, outs, cols, place, width, bufs, sems):
        self.spans, self.outs, self.place, self.width = spans, outs, place, width
        self.slots = cols - 1
        self.reduces = line_reduces(spans, parts, cols, place, width, bufs, sems[0], sems[1])
        self.gathers = line_gathers(spans, outs, cols, place, width, sems[2], sems[3])
        self.turns = len(spans) + 2 * self.slots

    def advance(self, number, step):
        which, first, size = self.spans[number]
        dst = self.outs[which]
        slots = self.slots
        if step < slots:
            self.reduces[number].step(step)
        elif step == slots:

            def store(value):
                dst[pl.ds(first, size), aligned(self.place, self.width)] = value.astype(BF)

            self.reduces[number].total(store)
            self.gathers[number].start(0)
        elif step < 2 * slots:
            self.gathers[number].arrive(step - slots - 1)
            self.gathers[number].start(step - slots)
        else:
            self.gathers[number].arrive(slots - 1)

    def turn(self, turn):
        for number in range(len(self.spans)):
            step = turn - number
            if 0 <= step <= 2 * self.slots:
                self.advance(number, step)

    def finish(self):
        for number in range(len(self.spans)):
            self.reduces[number].finish()
            self.gathers[number].finish()


def sum_branch(cols, part_img, part_txt, w_up, w_down):
    img, full = part_img.shape
    txt = part_txt.shape[0]
    width = full // cols
    spans = chunk_rows(img, txt, img // 4)
    count = len(spans)
    slots = cols - 1
    kinds = ("up", "down")
    weights = (w_up, w_down)
    subs = 2

    def kernel(*refs):
        parts, refs = refs[:2], refs[2:]
        shards, refs = refs[:2], refs[2:]
        outs, refs = refs[:2], refs[2:]
        fulls, refs = refs[:2], refs[2:]
        stages, refs = refs[:2], refs[2:]
        bufs, refs = refs[: 2 * count], refs[2 * count :]
        sems, (local_in, local_out, ws, wr) = refs[:4], refs[4:]
        place = lax.axis_index("col")
        line = LineSum(spans, parts, outs, cols, place, width, bufs, sems)
        flow = WeightFlow(kinds, shards, fulls, subs, ws, wr)
        owns = [
            OwnCopy(shards[n], stages[n], flow.own_view(n), local_in.at[n], local_out.at[n]) for n in range(2)
        ]
        for own in owns:
            own.begin()
        greet(others("row", 4) + others("col", cols) + [("dp", flow.mate)])
        flow.start(1)
        line.turn(0)
        flow.start(0)
        for own in owns:
            own.settle()
        pieces = len(flow.pieces)
        y_next = x_next = 0
        for turn in range(1, line.turns):
            line.turn(turn)
            while y_next < pieces and y_next * line.turns <= (turn - 2) * pieces:
                flow.relay_y(y_next)
                y_next += 1
                if y_next >= 2:
                    flow.relay_x(x_next)
                    x_next += 1
        while x_next < pieces:
            if y_next < pieces:
                flow.relay_y(y_next)
                y_next += 1
            flow.relay_x(x_next)
            x_next += 1
        flow.finish()
        line.finish()
        for own in owns:
            own.finish()

    return communicate(
        kernel,
        "sum_branch",
        2,
        out_shape=[struct(part_img.shape, BF), struct(part_txt.shape, BF)]
        + [struct(gathered_shape(k, w.shape), BF) for k, w in zip(kinds, weights)],
        in_specs=[VM, VM, ANY, ANY],
        out_specs=[VM, VM, ANY, ANY],
        scratch_shapes=[pltpu.VMEM(w.shape, BF) for w in weights]
        + line_buffers(spans, slots, width)
        + [pltpu.SemaphoreType.DMA((count, 2, slots))] * 4
        + [pltpu.SemaphoreType.DMA((2,))] * 2
        + [pltpu.SemaphoreType.DMA(WeightFlow.sem_shape(2, subs))] * 2,
    )(part_img, part_txt, *weights)


class Sibling:
    def __init__(self, pairs, ss, rs):
        self.pairs, self.ss, self.rs = pairs, ss, rs

    def copy(self, number):
        src, dst = self.pairs[number]
        return send(src, dst, self.ss.at[number], self.rs.at[number], "row", flip(lax.axis_index("row")))

    def start(self):
        for number in range(len(self.pairs)):
            self.copy(number).start()

    def land(self, *numbers):
        for number in numbers:
            self.copy(number).wait_recv()

    def finish(self):
        for number in range(len(self.pairs)):
            self.copy(number).wait_send()


def row_parts(ref, buf, core):
    size = ref.shape[1] // 4
    return [(ref.at[:, aligned(2 * y + core, size)], buf.at[y]) for y in range(2)]


def token_product(left_own, left_sib, right_own, right_sib):
    return lax.dot_general(left_own, right_own, OVER_FIRST, preferred_element_type=F32) + lax.dot_general(
        left_sib, right_sib, OVER_FIRST, preferred_element_type=F32
    )


def sum_hidden(cols, back, hidden, d_pre, act, d_mlp, first_hidden, attended):
    img, full = back[0].shape
    txt = back[1].shape[0]
    tokens = (img, txt)
    width = full // cols
    units = d_pre[0].shape[1]
    block = full // 4
    spans = chunk_rows(img, txt, img // 4)
    count = len(spans)
    slots = cols - 1
    tile = 512 if units % 512 == 0 else units

    def kernel(*refs):
        parts, hid, pre, acts, mlp, one, att = (refs[2 * n : 2 * n + 2] for n in range(7))
        refs = refs[14:]
        outs, refs = refs[:2], refs[2:]
        up_own, up_far, down_near = refs[:3]
        one_sib, att_sib = refs[3:5], refs[5:7]
        refs = refs[7:]
        hid_sib, pre_sib, act_sib, mlp_sib = (refs[2 * n : 2 * n + 2] for n in range(4))
        refs = refs[8:]
        down_own, far_out, far_in = refs[:3]
        refs = refs[3:]
        bufs, refs = refs[: 2 * count], refs[2 * count :]
        sems, (ss, rs, ys, yr) = refs[:4], refs[4:]
        place = lax.axis_index("col")
        row = lax.axis_index("row")
        core, y_of = lax.rem(row, 2), row // 2
        other = 1 - core
        far = flip_far(row)
        line = LineSum(spans, parts, outs, cols, place, width, bufs, sems)
        pairs = []
        for s in range(2):
            pairs += [(acts[s], act_sib[s])] + row_parts(mlp[s], mlp_sib[s], other)
        for s in range(2):
            pairs += [(pre[s], pre_sib[s])] + row_parts(hid[s], hid_sib[s], other)
        for s in range(2):
            pairs += [(att[s], att_sib[s])] + row_parts(one[s], one_sib[s], other)
        sibling = Sibling(pairs, ss, rs)
        greet(others("row", 4) + others("col", cols))
        line.turn(0)
        sibling.start()
        line.turn(1)

        def down(s, y, write):
            right_own = mlp[s][:, aligned(2 * y + core, block)]
            right_sib = mlp_sib[s][y]

            @pl.loop(0, units // tile)
            def _(at):
                cut = aligned(at, tile)
                write(cut, token_product(acts[s][:, cut], act_sib[s][:, cut], right_own, right_sib))

        def up(s, y, write):
            left_own = hid[s][:, aligned(2 * y + core, block)]
            left_sib = hid_sib[s][y]

            @pl.loop(0, units // tile)
            def _(at):
                cut = aligned(at, tile)
                write(cut, token_product(left_own, left_sib, pre[s][:, cut], pre_sib[s][:, cut]))

        def across(s):
            return send(far_out.at[s], far_in.at[s], ys.at[s], yr.at[s], "row", far)

        def down_to_far(s):
            sibling.land(3 * s, 3 * s + 1, 3 * s + 2)

            def write(cut, value):
                far_out[s, cut, :] = value.astype(BF)

            down(s, 1 - y_of, write)
            across(s).start()

        def down_here(s):
            def write(cut, value):
                down_own[s, cut, :] = value

            down(s, y_of, write)

        def up_to_far(s):
            sibling.land(6 + 3 * s, 7 + 3 * s, 8 + 3 * s)

            def write(cut, value):
                up_far[s, :, cut] = value.astype(BF)

            up(s, 1 - y_of, write)

        def up_here(s):
            def write(cut, value):
                up_own[s, :, cut] = value

            up(s, y_of, write)

        def down_sum(s):
            across(s).wait_recv()

            @pl.loop(0, units // tile)
            def _(at):
                cut = aligned(at, tile)
                down_near[s, cut, :] = (down_own[s, cut, :] + far_in[s, cut, :].astype(F32)).astype(BF)

        work = {
            1: lambda: down_to_far(0),
            2: lambda: down_to_far(1),
            3: lambda: down_here(0),
            4: lambda: (down_here(1), up_to_far(1)),
            5: lambda: up_to_far(0),
            6: lambda: up_here(0),
            7: lambda: up_here(1),
            8: lambda: down_sum(0),
        }
        for turn in range(1, line.turns):
            if turn > 1:
                line.turn(turn)
            if turn in work:
                work[turn]()
        down_sum(1)
        sibling.land(*range(12, 18))
        sibling.finish()
        for s in range(2):
            across(s).wait_send()
        line.finish()

    arrays = list(back) + list(hidden) + list(d_pre) + list(act) + list(d_mlp) + list(first_hidden) + list(attended)
    return communicate(
        kernel,
        "sum_hidden",
        3,
        out_shape=[struct(b.shape, BF) for b in back]
        + [
            struct((2, block, units), F32),
            struct((2, block, units), BF),
            struct((2, units, block), BF),
        ]
        + [struct((2, t, block), BF) for t in tokens]
        + [struct(a.shape, BF) for a in attended],
        in_specs=[VM] * 10 + [ANY] * 4,
        out_specs=[VM] * 5 + [ANY] * 4,
        scratch_shapes=[pltpu.VMEM((2, t, block), BF) for t in tokens]
        + [pltpu.VMEM((t, units), BF) for t in tokens]
        + [pltpu.VMEM((t, units), BF) for t in tokens]
        + [pltpu.VMEM((2, t, block), BF) for t in tokens]
        + [
            pltpu.VMEM((2, units, block), F32),
            pltpu.VMEM((2, units, block), BF),
            pltpu.VMEM((2, units, block), BF),
        ]
        + line_buffers(spans, slots, width)
        + [pltpu.SemaphoreType.DMA((count, 2, slots))] * 4
        + [pltpu.SemaphoreType.DMA((18,))] * 2
        + [pltpu.SemaphoreType.DMA((2,))] * 2,
    )(*arrays)


class GradFlow:
    def __init__(self, pods, product, outs, far_out, far_in, pod_out, pod_in, ys, yr, xs, xr):
        self.pods, self.product, self.outs = pods, product, outs
        self.far_out, self.far_in, self.pod_out, self.pod_in = far_out, far_in, pod_out, pod_in
        self.ys, self.yr, self.xs, self.xr = ys, yr, xs, xr
        row = lax.axis_index("row")
        self.y_of, self.far = row // 2, flip_far(row)

    @staticmethod
    def rounds(pods):
        return pods.bit_length() - 1

    @staticmethod
    def scratch(pods, count, shape):
        rounds = GradFlow.rounds(pods)
        return (
            [pltpu.VMEM((count,) + shape, BF)] * 2
            + [pltpu.VMEM((count, rounds) + shape, BF)] * 2
            + [pltpu.SemaphoreType.DMA((count,))] * 2
            + [pltpu.SemaphoreType.DMA((count, rounds))] * 2
        )

    def across(self, piece):
        return send(
            self.far_out.at[piece], self.far_in.at[piece], self.ys.at[piece], self.yr.at[piece], "row", self.far
        )

    def over(self, piece, turn):
        pod = lax.axis_index("dp")
        step = 2**turn
        peer = pod + step - 2 * step * lax.rem(pod // step, 2)
        return send(
            self.pod_out.at[piece, turn],
            self.pod_in.at[piece, turn],
            self.xs.at[piece, turn],
            self.xr.at[piece, turn],
            "dp",
            peer,
        )

    def to_far(self, piece):
        self.far_out[piece] = self.product(piece, 1 - self.y_of).astype(BF)
        self.across(piece).start()

    def here(self, piece):
        self.outs(piece)[...] = self.product(piece, self.y_of)

    def to_pod(self, piece):
        self.across(piece).wait_recv()
        self.pod_out[piece, 0] = (self.outs(piece)[...] + self.far_in[piece].astype(F32)).astype(BF)
        self.over(piece, 0).start()

    def done(self, piece):
        rounds = self.rounds(self.pods)
        for turn in range(rounds):
            self.over(piece, turn).wait_recv()
            total = self.pod_out[piece, turn].astype(F32) + self.pod_in[piece, turn].astype(F32)
            if turn == rounds - 1:
                self.outs(piece)[...] = total
            else:
                self.pod_out[piece, turn + 1] = total.astype(BF)
                self.over(piece, turn + 1).start()

    def finish(self, piece):
        self.across(piece).wait_send()
        for turn in range(self.rounds(self.pods)):
            self.over(piece, turn).wait_send()

    @staticmethod
    def friends(pods):
        pod = lax.axis_index("dp")
        found = []
        for turn in range(GradFlow.rounds(pods)):
            step = 2**turn
            found.append(("dp", pod + step - 2 * step * lax.rem(pod // step, 2)))
        return found


def sum_keys(pods, cols, d_key, d_value, part_img, part_txt, img, attended, attended_sib, d_branch):
    blocks, seqs, tokens, width = d_key.shape
    txt = tokens - img
    img_rows, full = part_img.shape
    block = full // 4
    spans = chunk_rows(img_rows, part_txt.shape[0], img_rows // 4)
    count = len(spans)
    slots = cols - 1
    lots = [(which, seq) for which in range(2) for seq in range(seqs)]
    lot_count = len(lots)

    def kernel(*refs):
        dk_ref, dv_ref = refs[:2]
        parts = refs[2:4]
        att, att_sib, bra = refs[4:6], refs[6:8], refs[8:10]
        kv_img, kv_txt = refs[10:12]
        line_out = refs[12:14]
        grad_ref = refs[14]
        near_in, far_out, far_in, ns, nr, fs, fr = refs[15:22]
        bra_sib = refs[22:24]
        ss, rs = refs[24:26]
        grad_scratch = refs[26:34]
        refs = refs[34:]
        bufs, refs = refs[: 2 * count], refs[2 * count :]
        rss, rsr = refs
        row = lax.axis_index("row")
        place = lax.axis_index("col")
        core = lax.rem(row, 2)
        sib, far = flip(row), flip_far(row)
        sources = (dk_ref, dv_ref)
        reduces = line_reduces(spans, parts, cols, place, width, bufs, rss, rsr)
        sibling = Sibling(
            [pair for s in range(2) for pair in row_parts(bra[s], bra_sib[s], 1 - core)], ss, rs
        )

        def product(s, y):
            return token_product(
                att[s][...], att_sib[s][...], bra[s][:, aligned(2 * y + core, block)], bra_sib[s][y]
            )

        grads = GradFlow(pods, product, lambda s: grad_ref.at[s], *grad_scratch)
        greet(others("row", 4) + others("col", cols) + GradFlow.friends(pods))

        def near(lot, number):
            which, seq = lots[lot]
            target = flip(far) if number == 0 else sib
            return send(
                sources[which].at[target, seq],
                near_in.at[lot, number],
                ns.at[lot, number],
                nr.at[lot, number],
                "row",
                sib,
            )

        def across(lot):
            return send(far_out.at[lot], far_in.at[lot], fs.at[lot], fr.at[lot], "row", far)

        for lot in range(lot_count):
            near(lot, 0).start()
        sibling.start()
        for lot in range(lot_count):
            near(lot, 1).start()

        def line_step(number, step):
            which, first, size = spans[number]
            dst = line_out[which]
            if step < slots:
                reduces[number].step(step)
            else:

                def store(value):
                    dst[pl.ds(first, size), :] = value

                reduces[number].total(store)

        def near_step(lot):
            which, seq = lots[lot]
            near(lot, 0).wait_recv()
            far_out[lot] = (sources[which][far, seq].astype(F32) + near_in[lot, 0].astype(F32)).astype(BF)
            across(lot).start()

        def far_step(lot):
            which, seq = lots[lot]
            near(lot, 1).wait_recv()
            across(lot).wait_recv()
            total = (
                sources[which][row, seq].astype(F32)
                + near_in[lot, 1].astype(F32)
                + far_in[lot].astype(F32)
            ).astype(BF)
            kv_img[which, seq] = total[:img]
            kv_txt[which, seq] = total[img:]

        for number in range(count):
            line_step(number, 0)
        for lot in range(lot_count):
            near_step(lot)
        sibling.land(0, 1, 2, 3)
        for s in range(2):
            grads.to_far(s)
        for turn in range(1, slots):
            for number in range(count):
                line_step(number, turn)
            if turn == 1:
                for s in range(2):
                    grads.here(s)
            far_step(turn - 1)
        for lot in range(slots - 1, lot_count):
            far_step(lot)
        for s in range(2):
            grads.to_pod(s)
        for number in range(count):
            line_step(number, slots)
        for s in range(2):
            grads.done(s)
        sibling.finish()
        for lot in range(lot_count):
            for number in range(2):
                near(lot, number).wait_send()
            across(lot).wait_send()
        for number in range(count):
            reduces[number].finish()
        for s in range(2):
            grads.finish(s)

    return communicate(
        kernel,
        "sum_keys",
        4,
        out_shape=[
            struct((2, seqs, img, width), BF),
            struct((2, seqs, txt, width), BF),
            struct((img_rows, width), F32),
            struct((part_txt.shape[0], width), F32),
            struct((2, width, block), F32),
        ],
        in_specs=[VM] * 10,
        out_specs=[VM] * 5,
        scratch_shapes=[
            pltpu.VMEM((lot_count, 2, tokens, width), BF),
            pltpu.VMEM((lot_count, tokens, width), BF),
            pltpu.VMEM((lot_count, tokens, width), BF),
            pltpu.SemaphoreType.DMA((lot_count, 2)),
            pltpu.SemaphoreType.DMA((lot_count, 2)),
            pltpu.SemaphoreType.DMA((lot_count,)),
            pltpu.SemaphoreType.DMA((lot_count,)),
        ]
        + [pltpu.VMEM((2, b.shape[0], block), BF) for b in d_branch]
        + [pltpu.SemaphoreType.DMA((4,))] * 2
        + GradFlow.scratch(pods, 2, (width, block))
        + line_buffers(spans, slots, width)
        + [pltpu.SemaphoreType.DMA((count, 2, slots))] * 2,
    )(d_key, d_value, part_img, part_txt, *attended, *attended_sib, *d_branch)


def sum_last(
    pods, cols, d_q, d_kv, qkv, hidden, hidden_sib, xs, cots, branch, d_two, mlp, stat_cols, tables, b_down, up_rows, ada
):
    seqs = tables.shape[2]
    tokens = [x.shape[0] for x in xs]
    counts = [t // seqs for t in tokens]
    width = xs[0].shape[1]
    full = width * cols
    block = full // 4
    spans = chunk_rows(tokens[0], tokens[1], tokens[0] // 4)
    count = len(spans)
    slots = cols - 1
    pieces = [(s, k) for s in range(2) for k in range(3)]
    lanes = tokens[0] + 128
    firsts = (0, tokens[0])
    mods_rows = 2 * seqs * 6
    up_count = up_rows.shape[0]
    pack_rows = mods_rows + 8 + up_count

    def kernel(*refs):
        takes = iter(refs)

        def two():
            return (next(takes), next(takes))

        dq, dkv = two(), two()
        qkv_ref = next(takes)
        hid, hid_sib, x_ref, cot_ref, bra, dtwo, mlp_ref, stat = (two() for _ in range(8))
        table_ref, down_ref, up_ref, ada_ref = (next(takes) for _ in range(4))
        out_ref, dx_ref = two(), two()
        grad_ref, every_ref, silu_ref = (next(takes) for _ in range(3))
        dq_sib, dkv_sib, parts, d_one, grown = (two() for _ in range(5))
        sums_mine, sums_in, pack_mine, pack_in, silu_mine, silu_in = (next(takes) for _ in range(6))
        ss, rs, ms, mr, ps, pr, es, er, cs, cr = (next(takes) for _ in range(10))
        grad_scratch = [next(takes) for _ in range(8)]
        bufs = [next(takes) for _ in range(2 * count)]
        rss, rsr = next(takes), next(takes)
        row = lax.axis_index("row")
        place = lax.axis_index("col")
        pod = lax.axis_index("dp")
        core = lax.rem(row, 2)
        mine = aligned(place, width)
        reduces = line_reduces(spans, parts, cols, place, width, bufs, rss, rsr)
        sibling = Sibling([pair for s in range(2) for pair in ((dq[s], dq_sib[s]), (dkv[s], dkv_sib[s]))], ss, rs)

        def projected(own, s, k):
            return own[0][s][...] if k == 0 else own[1][s][k - 1]

        def product(piece, y):
            s, k = pieces[piece]
            return token_product(
                hid[s][:, aligned(2 * y + core, block)],
                hid_sib[s][y],
                projected((dq, dkv), s, k),
                projected((dq_sib, dkv_sib), s, k),
            )

        def out_view(piece):
            s, k = pieces[piece]
            return grad_ref.at[s, k]

        grads = GradFlow(pods, product, out_view, *grad_scratch)
        greet(others("col", cols) + others("row", 4) + others("dp", pods))
        sibling.start()

        for number, (s, first, size) in enumerate(spans):
            rows = pl.ds(first, size)
            term = lax.dot_general(dq[s][rows, :], qkv_ref[s, 0], OVER_LAST, preferred_element_type=F32)
            for k in range(2):
                term = term + lax.dot_general(
                    dkv[s][k, rows, :], qkv_ref[s, k + 1], OVER_LAST, preferred_element_type=F32
                )
            parts[s][rows, :] = term.astype(BF)
            reduces[number].step(0)
        for s in range(2):
            sibling.land(2 * s, 2 * s + 1)
            for k in range(3):
                grads.to_far(3 * s + k)
        for number in range(count):
            reduces[number].step(1)
        for piece in range(6):
            grads.here(piece)

        def segment(s, q):
            return pl.ds(q * counts[s], counts[s])

        def modulation(s, q, position):
            return table_ref[place, s, q, pl.ds(position, 1), :]

        def put(index, value):
            pack_mine[pl.ds(index, 1), :] = value

        def over_tokens(value):
            return jnp.sum(value, axis=0, keepdims=True)

        def early(s):
            d_out = d_down = None
            for q in range(seqs):
                rows = segment(s, q)
                at = (s * seqs + q) * 6
                column = stat[s][rows, :]
                cot = cot_ref[s][rows, :].astype(F32)
                d_hidden = dtwo[s][rows, mine].astype(F32)
                attn = bra[s][rows, mine].astype(F32) + modulation(s, q, 6)
                gate_a, gate_m = modulation(s, q, 2), modulation(s, q, 5)
                middle = x_ref[s][rows, :].astype(F32) + gate_a * attn
                mlp_branch = mlp_ref[s][rows, :] + down_ref[pl.ds(s, 1), :]
                out_ref[s][rows, :] = (middle + gate_m * mlp_branch).astype(BF)
                normed = (middle - column[:, 2:3]) * column[:, 3:4]
                d_normed = d_hidden * (1.0 + modulation(s, q, 4))
                d_middle = cot + column[:, 3:4] * (d_normed - column[:, 4:5] - normed * column[:, 5:6])
                dx_ref[s][rows, :] = d_middle
                put(at + 2, over_tokens(d_middle * attn))
                put(at + 3, over_tokens(d_hidden))
                put(at + 4, over_tokens(d_hidden * normed))
                put(at + 5, over_tokens(cot * mlp_branch))
                first, second = over_tokens(d_middle * gate_a), over_tokens(cot * gate_m)
                d_out = first if d_out is None else d_out + first
                d_down = second if d_down is None else d_down + second
            put(mods_rows + 4 + s, d_out)
            put(mods_rows + 6 + s, d_down)
            put(mods_rows + 2 * s, over_tokens(dq[s][...].astype(F32)))
            put(mods_rows + 2 * s + 1, over_tokens(dkv[s][1].astype(F32)))

        pack_mine[pl.ds(mods_rows + 8, up_count), :] = up_ref[...]
        early(1)
        for number in range(count):
            for turn in range(2, slots):
                reduces[number].step(turn)
        early(0)
        grads.to_pod(0)
        grads.to_pod(1)
        for number, (s, first, size) in enumerate(spans):

            def store(value, s=s, first=first, size=size):
                d_one[s][pl.ds(first, size), :] = value

            reduces[number].total(store)

        one_row = lax.broadcasted_iota(jnp.int32, (8, width), 0)
        pick = [jnp.where(one_row == k, 1.0, 0.0).astype(F32) for k in range(2)]
        for s in range(2):
            for q in range(seqs):
                rows = segment(s, q)
                at = (s * seqs + q) * 6
                column = stat[s][rows, :]
                normed = (x_ref[s][rows, :].astype(F32) - column[:, 0:1]) * column[:, 1:2]
                d_hidden = d_one[s][rows, :]
                put(at, over_tokens(d_hidden))
                put(at + 1, over_tokens(d_hidden * normed))
                value = d_hidden * (1.0 + modulation(s, q, 1))
                d_one[s][rows, :] = value
                grown[s][rows, :] = value * normed
            exact = lax.Precision.HIGHEST
            sums_mine[:, pl.ds(firsts[s], tokens[s])] = lax.dot_general(
                pick[0], d_one[s][...], OVER_LAST, precision=exact, preferred_element_type=F32
            ) + lax.dot_general(pick[1], grown[s][...], OVER_LAST, precision=exact, preferred_element_type=F32)

        def small(step):
            return send(
                sums_mine, sums_in.at[step - 1], ms.at[step - 1], mr.at[step - 1], "col", lax.rem(place + step, cols)
            )

        for step in range(1, cols):
            small(step).start()

        def pack_copy(step):
            return send(
                pack_mine, pack_in.at[step - 1], ps.at[step - 1], pr.at[step - 1], "row", lax.rem(row + step, 4)
            )

        for step in range(1, 4):
            pack_copy(step).start()
        grads.to_pod(2)
        total = sums_mine[...]
        for step in range(1, cols):
            small(step).wait()
            total = total + sums_in[step - 1]
        lane = lax.broadcasted_iota(jnp.int32, (8, 128), 1)
        sublane = lax.broadcasted_iota(jnp.int32, (8, 128), 0)
        spread = jnp.where(sublane == lane // HD, 1.0 / full, 0.0).astype(F32)
        for s in range(2):
            means = lax.dot_general(
                total[:, firsts[s] : firsts[s] + tokens[s]],
                spread,
                OVER_FIRST,
                precision=lax.Precision.HIGHEST,
                preferred_element_type=F32,
            )
            column = stat[s][...]
            normed = (x_ref[s][...].astype(F32) - column[:, 0:1]) * column[:, 1:2]
            dx_ref[s][...] = dx_ref[s][...] + column[:, 1:2] * (
                d_one[s][...] - means[:, 0:1] - normed * means[:, HD : HD + 1]
            )
        grads.to_pod(3)

        def ordered(own, theirs, index, size):
            value = jnp.zeros_like(own)
            for number in range(size):
                gap = lax.rem(index - number + size, size)
                value = value + jnp.where(gap == 0, own, theirs[jnp.maximum(gap - 1, 0)])
            return value

        for step in range(1, 4):
            pack_copy(step).wait()
        packed = ordered(pack_mine[...], pack_in, row, 4)
        every_ref[pod] = packed

        def every_copy(step):
            at = every_ref.at[pod]
            return send(at, at, es.at[step - 1], er.at[step - 1], "dp", lax.rem(pod + step, pods))

        for step in range(1, pods):
            every_copy(step).start()
        d_silu = jnp.zeros((8, width), F32)
        for s in range(2):
            for k in range(6):
                rows = [packed[(s * seqs + q) * 6 + k : (s * seqs + q) * 6 + k + 1] for q in range(seqs)]
                value = jnp.concatenate(rows, axis=0)
                high = value.astype(BF)
                rest = value - high.astype(F32)
                mid = rest.astype(BF)
                low = (rest - mid.astype(F32)).astype(BF)
                terms = jnp.concatenate(
                    [high.astype(F32), mid.astype(F32), low.astype(F32), jnp.zeros((8 - 3 * seqs, width), F32)], axis=0
                ).astype(BF)
                d_silu = d_silu + lax.dot_general(terms, ada_ref[s, k], OVER_LAST, preferred_element_type=F32)
        silu_mine[...] = d_silu[:seqs] + d_silu[seqs : 2 * seqs] + d_silu[2 * seqs : 3 * seqs]

        def silu_copy(step):
            return send(
                silu_mine, silu_in.at[step - 1], cs.at[step - 1], cr.at[step - 1], "col", lax.rem(place + step, cols)
            )

        for step in range(1, cols):
            silu_copy(step).start()
        for piece in (4, 5):
            grads.to_pod(piece)
        for step in range(1, cols):
            silu_copy(step).wait()
        silu_ref[...] = ordered(silu_mine[...], silu_in, place, cols)
        for piece in range(6):
            grads.done(piece)
        for step in range(1, pods):
            source = lax.rem(pod - step + pods, pods)
            at = every_ref.at[source]
            send(at, at, es.at[step - 1], er.at[step - 1], "dp", source).wait_recv()
            every_copy(step).wait_send()
        sibling.finish()
        for number in range(count):
            reduces[number].finish()
        for piece in range(6):
            grads.finish(piece)

    arrays = (
        list(d_q)
        + list(d_kv)
        + [qkv]
        + list(hidden)
        + list(hidden_sib)
        + list(xs)
        + list(cots)
        + list(branch)
        + list(d_two)
        + list(mlp)
        + list(stat_cols)
        + [tables, b_down, up_rows, ada]
    )
    dma = pltpu.SemaphoreType.DMA
    return communicate(
        kernel,
        "sum_last",
        5,
        out_shape=[struct((t, width), BF) for t in tokens]
        + [struct((t, width), F32) for t in tokens]
        + [
            struct((2, 3, block, width), F32),
            struct((pods, pack_rows, width), F32),
            struct((seqs, width), F32),
        ],
        in_specs=[VM] * len(arrays),
        out_specs=[VM] * 7,
        scratch_shapes=[pltpu.VMEM(a.shape, BF) for a in d_q]
        + [pltpu.VMEM(a.shape, BF) for a in d_kv]
        + [pltpu.VMEM((t, full), BF) for t in tokens]
        + [pltpu.VMEM((t, width), F32) for t in tokens] * 2
        + [
            pltpu.VMEM((8, lanes), F32),
            pltpu.VMEM((slots, 8, lanes), F32),
            pltpu.VMEM((pack_rows, width), F32),
            pltpu.VMEM((3, pack_rows, width), F32),
            pltpu.VMEM((seqs, width), F32),
            pltpu.VMEM((slots, seqs, width), F32),
        ]
        + [dma((4,))] * 2
        + [dma((slots,))] * 2
        + [dma((3,))] * 2
        + [dma((pods - 1,))] * 2
        + [dma((slots,))] * 2
        + GradFlow.scratch(pods, 6, (block, width))
        + line_buffers(spans, slots, width)
        + [dma((count, 2, slots))] * 2,
    )(*arrays)


def gelu_pair(inputs):
    inner = GELU_ROOT * (inputs + GELU_CUBIC * inputs * inputs * inputs)
    tanh_value = jnp.tanh(inner)
    result = 0.5 * inputs * (1.0 + tanh_value)
    derivative = 0.5 * (1.0 + tanh_value) + 0.5 * inputs * (
        1.0 - tanh_value * tanh_value
    ) * GELU_ROOT * (1.0 + 3.0 * GELU_CUBIC * inputs * inputs)
    return (result, derivative)


def stats(values):
    mean = jnp.mean(values, axis=-1, keepdims=True)
    centred = values - mean
    inverse = lax.rsqrt(jnp.mean(centred * centred, axis=-1, keepdims=True) + EPSILON)
    return mean, inverse


def dot_f32(left, right):
    return jnp.einsum("td,de->te", left, right, preferred_element_type=F32)


def dot_back(left, right):
    return jnp.einsum("te,de->td", left, right, preferred_element_type=F32)


def dot_tokens(left, right):
    return jnp.einsum("td,te->de", left, right, preferred_element_type=F32)


def local(
    dp_count,
    row_count,
    col_count,
    x_img,
    x_txt,
    condition,
    w_qkv,
    b_qv,
    w_out,
    b_out,
    w_up,
    b_up,
    w_down,
    b_down,
    w_ada,
    b_ada,
    cot_img,
    cot_txt,
):
    seqs, img, width = x_img.shape
    txt = x_txt.shape[1]
    full = width * col_count
    counts = (img, txt)

    cond_wide = condition.astype(F32)
    cond_act = jax.nn.silu(cond_wide).astype(BF)
    ada = jnp.transpose(w_ada, (0, 2, 1, 3))
    table = jnp.einsum("sc,zkcd->zskd", cond_act, ada, preferred_element_type=F32)
    table = jnp.pad(table, ((0, 0), (0, 0), (0, 2), (0, 0)))
    bias_six = jnp.broadcast_to(b_ada[:, None], (2, seqs, 6, width))
    bias_rest = jnp.broadcast_to(b_out[:, None, None], (2, seqs, 2, width))
    *x_full, qkv_full, out_full, tables = prologue(
        col_count,
        x_img,
        x_txt,
        jnp.transpose(w_qkv, (0, 2, 1, 3)),
        w_out,
        table,
        jnp.concatenate([bias_six, bias_rest], axis=2),
    )
    wide = jnp.transpose(tables, (1, 2, 3, 0, 4)).reshape(2, seqs, 8, full)

    def mod(stream, position):
        return wide[stream, :, position][:, None, :]

    resid = [array.astype(F32) for array in x_full]
    stats_one = [stats(array) for array in resid]
    normed_one = [(resid[s] - stats_one[s][0]) * stats_one[s][1] for s in range(2)]
    hidden_one = [
        (normed_one[s] * (1.0 + mod(s, 1)) + mod(s, 0)).astype(BF).reshape(seqs * counts[s], full)
        for s in range(2)
    ]
    queries, keyed = [], []
    for s in range(2):
        shape = (seqs, counts[s], width)
        q = (dot_f32(hidden_one[s], qkv_full[s, 0]) + b_qv[s, 0]).astype(BF).reshape(shape)
        k = dot_f32(hidden_one[s], qkv_full[s, 1]).astype(BF).reshape(shape)
        v = (dot_f32(hidden_one[s], qkv_full[s, 2]) + b_qv[s, 1]).astype(BF).reshape(shape)
        queries.append(q)
        keyed.append(jnp.stack([k, v], axis=0))
    keys, *cot_full = gather_keys(col_count, keyed[0], keyed[1], cot_img, cot_txt)
    o_img, o_txt, lse = attend(queries[0], queries[1], keys)
    attended = [o_img.reshape(seqs * img, width), o_txt.reshape(seqs * txt, width)]
    out_terms = [dot_f32(attended[s], out_full[s]).astype(BF) for s in range(2)]
    *branch_sum, up_full, down_full = sum_branch(col_count, out_terms[0], out_terms[1], w_up, w_down)
    attn_branch = [
        branch_sum[s].reshape(seqs, counts[s], full).astype(F32) + mod(s, 6) for s in range(2)
    ]
    middle = [resid[s] + mod(s, 2) * attn_branch[s] for s in range(2)]
    stats_two = [stats(array) for array in middle]
    normed_two = [(middle[s] - stats_two[s][0]) * stats_two[s][1] for s in range(2)]
    hidden_two = [
        (normed_two[s] * (1.0 + mod(s, 4)) + mod(s, 3)).astype(BF).reshape(seqs * counts[s], full)
        for s in range(2)
    ]
    d_mlp_bf = [
        (cot_full[s].astype(F32) * mod(s, 5)).astype(BF).reshape(seqs * counts[s], full)
        for s in range(2)
    ]
    act, d_pre, d_pre_bf, down_terms, up_back = [], [], [], [], []
    for s in range(2):
        pre = dot_f32(hidden_two[s], up_full[s]) + b_up[s]
        value, slope = gelu_pair(pre)
        act.append(value.astype(BF))
        d_pre.append(dot_back(d_mlp_bf[s], down_full[s]) * slope)
        d_pre_bf.append(d_pre[s].astype(BF))
        up_back.append(dot_back(d_pre_bf[s], up_full[s]).astype(BF))
        down_terms.append(dot_f32(act[s], down_full[s]).astype(BF))

    d_two_img, d_two_txt, up_own, up_far, down_near, *paired = sum_hidden(
        col_count, up_back, hidden_two, d_pre_bf, act, d_mlp_bf, hidden_one, attended
    )
    hidden_pairs, attended_pairs = paired[:2], paired[2:]

    far_perm = [(r, (r + 2) % 4) for r in range(row_count)]

    def pod_sum(rounded):
        step = 1
        while step < dp_count:
            perm = [(d, d ^ step) for d in range(dp_count)]
            value = rounded.astype(F32) + lax.ppermute(rounded, "dp", perm).astype(F32)
            rounded = value.astype(BF)
            step *= 2
        return value

    grad_down = pod_sum(down_near)
    up_near = (up_own + lax.ppermute(up_far, "row", far_perm).astype(F32)).astype(BF)

    d_hidden_two = [d_two_img, d_two_txt]
    d_hidden_two = [
        d_hidden_two[s].reshape(seqs, counts[s], full).astype(F32) for s in range(2)
    ]
    d_branch_bf, stat_cols = [], []
    for s in range(2):
        grown = d_hidden_two[s] * (1.0 + mod(s, 4))
        first = jnp.mean(grown, axis=-1, keepdims=True)
        second = jnp.mean(grown * normed_two[s], axis=-1, keepdims=True)
        d_middle = cot_full[s].astype(F32) + stats_two[s][1] * (grown - first - normed_two[s] * second)
        d_branch_bf.append((d_middle * mod(s, 2)).astype(BF).reshape(seqs * counts[s], full))
        columns = [*stats_one[s], *stats_two[s], first, second, jnp.zeros_like(first), jnp.zeros_like(first)]
        stat_cols.append(jnp.concatenate(columns, axis=-1).reshape(seqs * counts[s], 8))
    d_att = [
        dot_back(d_branch_bf[s], out_full[s]).astype(BF).reshape(seqs, counts[s], width)
        for s in range(2)
    ]
    dq_img, dq_txt, d_key, d_value = attend_back(
        queries[0], queries[1], keys, o_img, o_txt, d_att[0], d_att[1], lse
    )
    d_key, d_value, up_near = lax.optimization_barrier((d_key, d_value, up_near))
    grad_up = pod_sum(up_near)
    kv_img, kv_txt, mlp_img, mlp_txt, grad_out = sum_keys(
        dp_count,
        col_count,
        d_key,
        d_value,
        down_terms[0],
        down_terms[1],
        img,
        attended,
        attended_pairs,
        d_branch_bf,
    )

    flat = [(seqs * c, width) for c in counts]
    up_rows = jnp.concatenate([jnp.sum(d_pre[s], axis=0).reshape(-1, width) for s in range(2)], axis=0)
    out_img, out_txt, dx_img, dx_txt, grad_qkv, every, d_silu = sum_last(
        dp_count,
        col_count,
        [dq_img.reshape(flat[0]), dq_txt.reshape(flat[1])],
        [kv_img.reshape((2,) + flat[0]), kv_txt.reshape((2,) + flat[1])],
        qkv_full,
        hidden_one,
        hidden_pairs,
        [x_img.reshape(flat[0]), x_txt.reshape(flat[1])],
        [cot_img.reshape(flat[0]), cot_txt.reshape(flat[1])],
        branch_sum,
        [d_two_img, d_two_txt],
        [mlp_img, mlp_txt],
        stat_cols,
        tables,
        b_down,
        up_rows,
        ada,
    )
    grad_qkv = jnp.transpose(grad_qkv, (0, 2, 1, 3))
    mods_count = 2 * seqs * 6
    rest = jnp.sum(every[:, mods_count:], axis=0)
    grad_bqv = rest[:4].reshape(2, 2, width)
    grad_bout = rest[4:6]
    grad_bdown = rest[6:8]
    grad_bup = rest[8:].reshape(2, -1)
    all_mods = every[:, :mods_count].reshape(dp_count, 2, seqs, 6, width)
    all_cond = lax.all_gather(cond_act, "dp", axis=0, tiled=False).astype(F32)
    grad_ada = jnp.einsum(
        "psc,pzskd->zkcd", all_cond, all_mods, precision=lax.Precision.HIGHEST
    )
    grad_ada = jnp.transpose(grad_ada, (0, 2, 1, 3))
    grad_bada = jnp.sum(all_mods, axis=(0, 2))
    sigmoid_cond = jax.nn.sigmoid(cond_wide)
    d_condition = d_silu * sigmoid_cond * (1.0 + cond_wide * (1.0 - sigmoid_cond))
    return (
        out_img.reshape(x_img.shape),
        out_txt.reshape(x_txt.shape),
        dx_img.reshape(x_img.shape),
        dx_txt.reshape(x_txt.shape),
        d_condition,
        grad_qkv,
        grad_bqv,
        grad_out,
        grad_bout,
        grad_up,
        grad_bup,
        grad_down,
        grad_bdown,
        grad_ada,
        grad_bada,
    )


def solution(mesh):
    placed = (
        P("dp", "row", "col"),
        P("dp", "row", "col"),
        P("dp", "row"),
        P(None, "row", None, "col"),
        P(None, None, "col"),
        P(None, "col", "row"),
        P(None, "col"),
        P(None, "row", "col"),
        P(None, "col"),
        P(None, "col", "row"),
        P(None, "col"),
        P(None, "row", None, "col"),
        P(None, None, "col"),
        P("dp", "row", "col"),
        P("dp", "row", "col"),
    )
    return jax.shard_map(
        partial(local, mesh.shape["dp"], mesh.shape["row"], mesh.shape["col"]),
        mesh=mesh,
        in_specs=placed,
        out_specs=(
            P("dp", "row", "col"),
            P("dp", "row", "col"),
            P("dp", "row", "col"),
            P("dp", "row", "col"),
            P("dp", "row"),
            P(None, "row", None, "col"),
            P(None, None, "col"),
            P(None, "col", "row"),
            P(None, "col"),
            P(None, "row", "col"),
            P(None, "col"),
            P(None, "col", "row"),
            P(None, "col"),
            P(None, "row", None, "col"),
            P(None, None, "col"),
        ),
        check_vma=False,
    )
```

```python
import jax
import jax.numpy as jnp
from jax import lax
from jax.experimental import pallas as pl
from jax.experimental.pallas import tpu as pltpu
from jax.sharding import PartitionSpec as P


HD = 64
EPSILON = 1e-06
GELU_ROOT = 0.7978845608028654
GELU_CUBIC = 0.044715
BF = jnp.bfloat16
F32 = jnp.float32
MESH = pl.DeviceIdType.MESH
ANY = pl.BlockSpec(memory_space=pl.ANY)
VM = pl.BlockSpec(memory_space=pltpu.VMEM)
VMEM_LIMIT = 60 * 1024 * 1024


def struct(shape, dtype):
    return jax.ShapeDtypeStruct(shape, dtype)


def aligned(index, size):
    return pl.ds(pl.multiple_of(index * size, size), size)


def send(src, dst, send_sem, recv_sem, axis, index):
    return pltpu.make_async_remote_copy(
        src_ref=src,
        dst_ref=dst,
        send_sem=send_sem,
        recv_sem=recv_sem,
        device_id={axis: index},
        device_id_type=MESH,
    )


def flip(index):
    return index + 1 - 2 * lax.rem(index, 2)


def flip_far(index):
    return lax.rem(index + 2, 4)


def greet(pairs):
    barrier = pltpu.get_barrier_semaphore()
    for axis, index in pairs:
        pl.semaphore_signal(barrier, inc=1, device_id={axis: index}, device_id_type=MESH)
    pl.semaphore_wait(barrier, len(pairs))


def others(axis, count):
    me = lax.axis_index(axis)
    return [(axis, lax.rem(me + step, count)) for step in range(1, count)]


class LineGather:
    def __init__(self, view, count, place, send_sems, recv_sems):
        self.view, self.count, self.place = view, count, place
        self.send_sems, self.recv_sems = send_sems, recv_sems

    def copy(self, side, step, arriving):
        place = self.place
        if side == 0:
            block = place - step - (1 if arriving else 0)
            peer = place + 1
        else:
            block = place + step + (1 if arriving else 0)
            peer = place - 1
        view = self.view(block)
        return send(
            view, view, self.send_sems.at[side, step], self.recv_sems.at[side, step], "col", peer
        )

    def sends(self, side, step):
        if side == 0:
            return jnp.logical_and(self.place - step >= 0, self.place < self.count - 1)
        return jnp.logical_and(self.place + step <= self.count - 1, self.place > 0)

    def arrives(self, side, step):
        if side == 0:
            return self.place - 1 - step >= 0
        return self.place + 1 + step <= self.count - 1

    def start(self, step):
        for side in range(2):

            @pl.when(self.sends(side, step))
            def _():
                self.copy(side, step, False).start()

    def arrive(self, step):
        for side in range(2):

            @pl.when(self.arrives(side, step))
            def _():
                self.copy(side, step, True).wait_recv()

    def finish(self):
        for step in range(self.count - 1):
            for side in range(2):

                @pl.when(self.sends(side, step))
                def _():
                    self.copy(side, step, False).wait_send()


class LineReduce:
    def __init__(self, load, count, place, out_bufs, in_bufs, send_sems, recv_sems):
        self.load, self.count, self.place = load, count, place
        self.out_bufs, self.in_bufs = out_bufs, in_bufs
        self.send_sems, self.recv_sems = send_sems, recv_sems

    def copy(self, side, slot):
        peer = self.place + 1 if side == 0 else self.place - 1
        return send(
            self.out_bufs.at[side, slot],
            self.in_bufs.at[side, slot],
            self.send_sems.at[side, slot],
            self.recv_sems.at[side, slot],
            "col",
            peer,
        )

    def has_behind(self, side):
        return self.place > 0 if side == 0 else self.place < self.count - 1

    def target(self, side, slot):
        return self.place + 1 + slot if side == 0 else self.place - 1 - slot

    def sends(self, side, slot):
        target = self.target(side, slot)
        return target <= self.count - 1 if side == 0 else target >= 0

    def step(self, number):
        slot = self.count - 2 - number
        for side in range(2):

            @pl.when(self.sends(side, slot))
            def _():
                target = self.target(side, slot)
                if slot < self.count - 2:

                    @pl.when(self.has_behind(side))
                    def _():
                        self.copy(side, slot + 1).wait_recv()
                        self.out_bufs[side, slot] = (
                            self.load(target).astype(F32) + self.in_bufs[side, slot + 1].astype(F32)
                        ).astype(BF)

                    @pl.when(jnp.logical_not(self.has_behind(side)))
                    def _():
                        self.out_bufs[side, slot] = self.load(target)

                else:
                    self.out_bufs[side, slot] = self.load(target)
                self.copy(side, slot).start()

    def total(self, store):
        own = self.load(self.place).astype(F32)

        @pl.when(self.place == 0)
        def _():
            self.copy(1, 0).wait_recv()
            store(own + self.in_bufs[1, 0].astype(F32))

        @pl.when(self.place == self.count - 1)
        def _():
            self.copy(0, 0).wait_recv()
            store(own + self.in_bufs[0, 0].astype(F32))

        @pl.when(jnp.logical_and(self.place > 0, self.place < self.count - 1))
        def _():
            self.copy(0, 0).wait_recv()
            self.copy(1, 0).wait_recv()
            store(own + self.in_bufs[0, 0].astype(F32) + self.in_bufs[1, 0].astype(F32))

    def finish(self):
        for slot in range(self.count - 1):
            for side in range(2):

                @pl.when(self.sends(side, slot))
                def _():
                    self.copy(side, slot).wait_send()


def communicate(kernel, collective_id, **kwargs):
    return pl.pallas_call(
        kernel,
        compiler_params=pltpu.CompilerParams(
            collective_id=collective_id, has_side_effects=True, vmem_limit_bytes=VMEM_LIMIT
        ),
        **kwargs,
    )


class WeightFlow:
    def __init__(self, kinds, streams, shards, fulls, subs, send_sems, recv_sems):
        self.kinds, self.streams, self.shards, self.fulls, self.subs = kinds, streams, shards, fulls, subs
        self.send_sems, self.recv_sems = send_sems, recv_sems
        self.pieces = WeightFlow.listed(streams, subs)
        self.row = lax.axis_index("row")
        self.half = lax.rem(lax.axis_index("dp"), 2)
        self.mate = flip(lax.axis_index("dp"))
        self.sib, self.far = flip(self.row), flip_far(self.row)

    @staticmethod
    def listed(streams, subs):
        return [(n, s, u) for n in range(len(streams)) for s in streams[n] for u in range(subs)]

    @staticmethod
    def sem_shape(streams, subs):
        return (len(WeightFlow.listed(streams, subs)), 5)

    def split(self, depth, sub, part):
        if part is None:
            size = depth // self.subs
            return pl.ds(sub * size, size)
        size = depth // (2 * self.subs)
        return aligned(2 * sub + part, size)

    def view(self, piece, block, part):
        number, stream, sub = self.pieces[piece]
        kind, ref, shard = self.kinds[number], self.fulls[number], self.shards[number]
        stream -= self.streams[number][0]
        if kind == "qkv" or kind == "up":
            depth = shard.shape[-2]
            if part is None:
                size = depth // self.subs
                rows = aligned(block * self.subs + sub, size)
            else:
                rows = aligned(block * 2 * self.subs + 2 * sub + part, depth // (2 * self.subs))
            return ref.at[stream, :, rows, :] if kind == "qkv" else ref.at[stream, rows, :]
        return ref.at[stream, self.split(shard.shape[1], sub, part), aligned(block, shard.shape[2])]

    def source(self, piece, part):
        number, stream, sub = self.pieces[piece]
        ref = self.shards[number]
        rows = self.split(ref.shape[-2], sub, part)
        return ref.at[stream, :, rows, :] if self.kinds[number] == "qkv" else ref.at[stream, rows, :]

    def copy(self, piece, kind):
        sems = (self.send_sems.at[piece, kind], self.recv_sems.at[piece, kind])
        if kind == 0:
            return send(self.source(piece, None), self.view(piece, self.row, None), *sems, "row", self.sib)
        if kind == 1:
            return send(self.source(piece, self.half), self.view(piece, self.row, self.half), *sems, "row", self.far)
        at = self.view(piece, self.far, 1 - self.half if kind == 4 else self.half)
        if kind == 2:
            return send(at, at, *sems, "dp", self.mate)
        return send(at, at, *sems, "row", self.sib)

    def land(self, piece, kind):
        if kind == 0:
            at = self.view(piece, self.sib, None)
        elif kind == 1:
            at = self.view(piece, self.far, self.half)
        elif kind == 2:
            at = self.view(piece, self.far, 1 - self.half)
        elif kind == 3:
            at = self.view(piece, flip(self.far), self.half)
        else:
            at = self.view(piece, flip(self.far), 1 - self.half)
        send(at, at, self.send_sems.at[piece, kind], self.recv_sems.at[piece, kind], "row", self.sib).wait_recv()

    def start(self, kind):
        for piece in range(len(self.pieces)):
            self.copy(piece, kind).start()

    def relay_y(self, piece):
        self.land(piece, 1)
        self.copy(piece, 2).start()
        self.copy(piece, 3).start()

    def relay_x(self, piece):
        self.land(piece, 2)
        self.copy(piece, 4).start()

    def finish(self):
        for piece in range(len(self.pieces)):
            for kind in (0, 3, 4):
                self.land(piece, kind)
        for piece in range(len(self.pieces)):
            for kind in range(5):
                self.copy(piece, kind).wait_send()

    def own_view(self, number):
        kind, ref, shard = self.kinds[number], self.fulls[number], self.shards[number]
        if kind == "qkv":
            return ref.at[:, :, aligned(self.row, shard.shape[2]), :]
        if kind == "up":
            return ref.at[:, aligned(self.row, shard.shape[1]), :]
        return ref.at[:, :, aligned(self.row, shard.shape[2])]


def gathered_shape(kind, shape):
    if kind == "qkv":
        return shape[:2] + (shape[2] * 4, shape[3])
    if kind == "up":
        return (shape[0], shape[1] * 4, shape[2])
    return shape[:2] + (shape[2] * 4,)


class OwnCopy:
    def __init__(self, src, stage, dst, sem_in, sem_out):
        self.first = pltpu.make_async_copy(src, stage, sem_in)
        self.second = pltpu.make_async_copy(stage, dst, sem_out)

    def begin(self):
        self.first.start()

    def settle(self):
        self.first.wait()
        self.second.start()

    def finish(self):
        self.second.wait()


def line_from(shard, full, width, cols, place, zs, zr):
    def at(block):
        return full.at[:, :, aligned(block, width)]

    line = LineGather(at, cols, place, zs, zr)

    def first():
        for side in range(2):
            peer = place + 1 if side == 0 else place - 1

            @pl.when(line.sends(side, 0))
            def _():
                send(shard, at(place), zs.at[side, 0], zr.at[side, 0], "col", peer).start()

    return line, first, at(place)


def prologue(pods, cols, x_img, x_txt, qkv, out, table, bias, cond):
    shards = (x_img, x_txt, qkv, out)
    width = x_img.shape[2]
    rows = 4
    kinds, streams = ("qkv", "out"), ((0, 1), (0, 1))
    full_shapes = [s.shape[:2] + (s.shape[2] * cols,) for s in shards[:2]]
    full_shapes += [gathered_shape(k, s.shape) for k, s in zip(kinds, shards[2:])]
    table_shape = table.shape

    def kernel(*refs):
        shard = refs[:4]
        table_ref, bias_ref, cond_ref = refs[4:7]
        full = refs[7:11]
        mods_ref, every_cond = refs[11:13]
        stage = refs[13:17]
        parts = refs[17]
        local_in, local_out, zs, zr, ws, wr, ms, mr, cs, cr = refs[18:]
        pod = lax.axis_index("dp")
        place = lax.axis_index("col")
        row = lax.axis_index("row")
        flow = WeightFlow(kinds, streams, shard[2:], full[2:], 1, ws, wr)
        lines = [line_from(shard[n], full[n], width, cols, place, zs.at[n], zr.at[n]) for n in range(2)]
        owns = [OwnCopy(shard[n], stage[n], lines[n][2], local_in.at[n], local_out.at[n]) for n in range(2)]
        owns += [
            OwnCopy(shard[2 + n], stage[2 + n], flow.own_view(n), local_in.at[2 + n], local_out.at[2 + n])
            for n in range(2)
        ]
        for own in owns:
            own.begin()
        greet(others("row", rows) + others("col", cols) + others("dp", pods))

        def cond_copy(step):
            return send(
                cond_ref, every_cond.at[pod], cs.at[step - 1], cr.at[step - 1], "dp", lax.rem(pod + step, pods)
            )

        for step in range(1, pods):
            cond_copy(step).start()
        every_cond[pod] = cond_ref[...]

        def part_copy(step):
            return send(
                table_ref, parts.at[step - 1], ms.at[step - 1], mr.at[step - 1], "row", lax.rem(row + step, rows)
            )

        for step in range(1, rows):
            part_copy(step).start()
        for _, first, _ in lines:
            first()
        flow.start(1)
        flow.start(0)
        for step in range(1, rows):
            part_copy(step).wait()
        total = bias_ref[...]
        for index in range(rows):
            gap = lax.rem(row - index + rows, rows)
            theirs = parts[jnp.maximum(gap - 1, 0)]
            total = total + jnp.where(gap == 0, table_ref[...], theirs)
        mods_ref[place] = total

        def mod_copy(step):
            return send(
                mods_ref.at[place],
                mods_ref.at[place],
                ms.at[rows - 2 + step],
                mr.at[rows - 2 + step],
                "col",
                lax.rem(place + step, cols),
            )

        for step in range(1, cols):
            mod_copy(step).start()
        for own in owns:
            own.settle()
        flow.relay_y(0)
        for line, _, _ in lines:
            line.arrive(0)
            line.start(1)
        flow.relay_y(1)
        flow.relay_x(0)
        for step in range(2, cols - 1):
            for line, _, _ in lines:
                line.arrive(step - 1)
                line.start(step)
        flow.relay_y(2)
        flow.relay_x(1)
        flow.relay_y(3)
        flow.relay_x(2)
        flow.relay_x(3)
        for line, _, _ in lines:
            line.arrive(cols - 2)
        for step in range(1, cols):
            source_place = lax.rem(place - step + cols, cols)
            at = mods_ref.at[source_place]
            send(at, at, ms.at[rows - 2 + step], mr.at[rows - 2 + step], "col", source_place).wait_recv()
            mod_copy(step).wait_send()
        for line, _, _ in lines:
            line.finish()
        flow.finish()
        for own in owns:
            own.finish()
        for step in range(1, pods):
            source = lax.rem(pod - step + pods, pods)
            at = every_cond.at[source]
            send(at, at, cs.at[step - 1], cr.at[step - 1], "dp", source).wait_recv()
            cond_copy(step).wait_send()

    return communicate(
        kernel,
        0,
        out_shape=[struct(s, BF) for s in full_shapes]
        + [struct((cols,) + table_shape, F32), struct((pods,) + cond.shape, F32)],
        in_specs=[ANY] * 4 + [VM] * 3,
        out_specs=[ANY] * 4 + [VM] * 2,
        scratch_shapes=[pltpu.VMEM(s.shape, BF) for s in shards]
        + [
            pltpu.VMEM((rows - 1,) + table_shape, F32),
            pltpu.SemaphoreType.DMA((4,)),
            pltpu.SemaphoreType.DMA((4,)),
            pltpu.SemaphoreType.DMA((2, 2, cols - 1)),
            pltpu.SemaphoreType.DMA((2, 2, cols - 1)),
            pltpu.SemaphoreType.DMA(WeightFlow.sem_shape(streams, 1)),
            pltpu.SemaphoreType.DMA(WeightFlow.sem_shape(streams, 1)),
            pltpu.SemaphoreType.DMA((rows + cols - 2,)),
            pltpu.SemaphoreType.DMA((rows + cols - 2,)),
            pltpu.SemaphoreType.DMA((pods - 1,)),
            pltpu.SemaphoreType.DMA((pods - 1,)),
        ],
    )(*shards, table, bias, cond)


def front(cols, x_full, wide, qkv, b_qv, cots, w_up):
    seqs = wide.shape[1]
    full = wide.shape[3]
    width = full // cols
    tokens = [x.shape[0] for x in x_full]
    counts = [t // seqs for t in tokens]
    joint = sum(counts)
    lanes = 2 * HD
    pairs = width // lanes
    scale = HD ** (-0.5)
    kinds, streams, subs = ("up",), ((0,),), 2
    up_shape = (1,) + gathered_shape("up", w_up.shape)[1:]
    lots = [(which, q) for which in range(2) for q in range(seqs)]
    over_last = (((1,), (1,)), ((), ()))

    def kernel(*refs):
        takes = iter(refs)

        def two():
            return (next(takes), next(takes))

        x_any = two()
        wide_ref, qkv_any, bias_ref = (next(takes) for _ in range(3))
        cot_refs = two()
        up_shard = next(takes)
        hidden, queries = two(), two()
        keys = next(takes)
        attended = two()
        lse_ref = next(takes)
        cot_full = two()
        up_full = next(takes)
        x_ref = two()
        qkv_ref = next(takes)
        stage_cot = two()
        stage_up = next(takes)
        loads, local, ks, kr, zs, zr, ws, wr = (next(takes) for _ in range(8))
        row = lax.axis_index("row")
        place = lax.axis_index("col")
        sib, far = flip(row), flip_far(row)
        x_loads = [pltpu.make_async_copy(x_any[s], x_ref[s], loads.at[s]) for s in range(2)]
        w_loads = [
            pltpu.make_async_copy(qkv_any.at[s, k], qkv_ref.at[s, k], loads.at[2 + 3 * s + k])
            for k in (1, 2, 0)
            for s in range(2)
        ]
        for load in x_loads + w_loads:
            load.start()
        flow = WeightFlow(kinds, streams, (up_shard,), (up_full,), subs, ws, wr)
        lines = [line_from(cot_refs[n], cot_full[n], width, cols, place, zs.at[n], zr.at[n]) for n in range(2)]
        owns = [OwnCopy(cot_refs[n], stage_cot[n], lines[n][2], local.at[n], local.at[2 + n]) for n in range(2)]
        owns.append(OwnCopy(up_shard.at[pl.ds(0, 1)], stage_up, flow.own_view(0), local.at[4], local.at[5]))
        for own in owns:
            own.begin()
        greet(others("row", 4) + others("col", cols) + [("dp", flow.mate)])
        for _, first, _ in lines:
            first()
        flow.copy(0, 1).start()

        for s in range(2):
            x_loads[s].wait()
            rows = min(64, counts[s])
            for q in range(seqs):
                shift, grow = wide_ref[s, q, 0:1, :], 1.0 + wide_ref[s, q, 1:2, :]

                @pl.loop(0, counts[s] // rows)
                def _(at):
                    cut = pl.ds(pl.multiple_of(q * counts[s] + at * rows, rows), rows)
                    resid = x_ref[s][cut, :].astype(F32)
                    mean, inverse = stats(resid)
                    hidden[s][cut, :] = ((resid - mean) * inverse * grow + shift).astype(BF)

        def key_copy(kind, lot):
            which, q = lots[lot]
            at = keys.at[far if kind == 2 else row, which, q]
            return send(at, at, ks.at[kind, lot], kr.at[kind, lot], "row", far if kind == 0 else sib)

        def key_land(kind, lot):
            which, q = lots[lot]
            at = keys.at[(far, sib, flip(far))[kind], which, q]
            send(at, at, ks.at[kind, lot], kr.at[kind, lot], "row", sib).wait_recv()

        def project(s, k):
            return jnp.dot(hidden[s][...], qkv_ref[s, k], preferred_element_type=F32)

        for which in range(2):
            for s in range(2):
                w_loads[2 * which + s].wait()
                value = project(s, which + 1)
                if which == 1:
                    value = value + bias_ref[s, 1:2, :]
                value = value.astype(BF)
                first = 0 if s == 0 else counts[0]
                for q in range(seqs):
                    keys[row, which, q, pl.ds(first, counts[s]), :] = value[q * counts[s] : (q + 1) * counts[s]]
            for q in range(seqs):
                key_copy(0, which * seqs + q).start()
                key_copy(1, which * seqs + q).start()
        for piece in range(1, len(flow.pieces)):
            flow.copy(piece, 1).start()
        for own in owns:
            own.settle()
        for s in range(2):
            w_loads[4 + s].wait()
            queries[s][...] = (project(s, 0) + bias_ref[s, 0:1, :]).astype(BF)
        flow.start(0)
        for lot in range(len(lots)):
            key_land(0, lot)
            key_copy(2, lot).start()
            if lot == 0:
                flow.relay_y(0)
                for line, _, _ in lines:
                    line.arrive(0)
                    line.start(1)
        for line, _, _ in lines:
            for step in range(2, cols - 1):
                line.arrive(step - 1)
                line.start(step)
        flow.relay_x(0)
        for lot in range(len(lots)):
            key_land(1, lot)
            key_land(2, lot)

        low = lax.broadcasted_iota(jnp.int32, (joint, lanes), 1) < HD
        for q in range(seqs):
            img_rows, txt_rows = pl.ds(q * counts[0], counts[0]), pl.ds(q * counts[1], counts[1])

            @pl.loop(0, pairs)
            def _(pair):
                cut = aligned(pair, lanes)
                asked = jnp.concatenate([queries[0][img_rows, cut], queries[1][txt_rows, cut]], axis=0)
                key_block = keys[:, 0, q, :, cut].reshape(4 * joint, lanes)
                value_block = keys[:, 1, q, :, cut].reshape(4 * joint, lanes)
                results, sums = [], []
                for head in range(2):
                    mine = low if head == 0 else jnp.logical_not(low)
                    chosen = jnp.where(mine, asked, jnp.zeros_like(asked))
                    scores = (
                        lax.dot_general(chosen, key_block, over_last, preferred_element_type=F32) * scale
                    )
                    highest = jnp.max(scores, axis=-1, keepdims=True)
                    grown = jnp.exp(scores - highest)
                    total = jnp.sum(grown, axis=-1, keepdims=True)
                    weights = (grown * (1.0 / total)).astype(BF)
                    results.append(jnp.dot(weights, value_block, preferred_element_type=F32))
                    sums.append(jnp.broadcast_to(highest + jnp.log(total), (joint, lanes)))
                result = jnp.where(low, results[0], results[1]).astype(BF)
                attended[0][img_rows, cut] = result[: counts[0]]
                attended[1][txt_rows, cut] = result[counts[0] :]
                lse_ref[q, pair] = jnp.where(low, sums[0], sums[1])

            if q == 0:
                for piece in range(1, len(flow.pieces)):
                    flow.relay_y(piece)
        for piece in range(1, len(flow.pieces)):
            flow.relay_x(piece)
        for line, _, _ in lines:
            line.arrive(cols - 2)
        for line, _, _ in lines:
            line.finish()
        for lot in range(len(lots)):
            for kind in range(3):
                key_copy(kind, lot).wait_send()
        flow.finish()
        for own in owns:
            own.finish()

    dma = pltpu.SemaphoreType.DMA
    return communicate(
        kernel,
        1,
        out_shape=[struct((t, full), BF) for t in tokens]
        + [struct((t, width), BF) for t in tokens]
        + [struct((4, 2, seqs, joint, width), BF)]
        + [struct((t, width), BF) for t in tokens]
        + [struct((seqs, pairs, joint, lanes), F32)]
        + [struct(c.shape[:2] + (full,), BF) for c in cots]
        + [struct(up_shape, BF)],
        in_specs=[ANY, ANY, VM, ANY, VM, ANY, ANY, ANY],
        out_specs=[VM] * 8 + [ANY] * 3,
        scratch_shapes=[pltpu.VMEM(x.shape, BF) for x in x_full]
        + [pltpu.VMEM(qkv.shape, BF)]
        + [pltpu.VMEM(c.shape, BF) for c in cots]
        + [
            pltpu.VMEM((1,) + w_up.shape[1:], BF),
            dma((8,)),
            dma((6,)),
            dma((3, len(lots))),
            dma((3, len(lots))),
            dma((2, 2, cols - 1)),
            dma((2, 2, cols - 1)),
            dma(WeightFlow.sem_shape(streams, subs)),
            dma(WeightFlow.sem_shape(streams, subs)),
        ],
    )(*x_full, wide, qkv, b_qv, *cots, w_up)


def attend_back(q, keys, attended, lse, x_full, cot_full, branch, d_two, wide, out_full):
    seqs, img, width = q[0].shape
    txt = q[1].shape[1]
    counts = (img, txt)
    tokens = img + txt
    blocks = keys.shape[0]
    pairs = width // (2 * HD)
    lanes = 2 * HD
    full = x_full[0].shape[2]
    scale = HD ** (-0.5)
    over_last = (((1,), (1,)), ((), ()))
    over_first = (((0,), (0,)), ((), ()))

    def kernel(*refs):
        takes = iter(refs)

        def two():
            return (next(takes), next(takes))

        q_ref, o_ref, x_ref, cot_ref, bra, dtwo = (two() for _ in range(6))
        k_ref, v_ref, lse_ref, wide_ref, out_ref = (next(takes) for _ in range(5))
        dq, d_branch, stat = (two() for _ in range(3))
        dk_ref, dv_ref = next(takes), next(takes)

        @pl.when(pl.program_id(1) == 0)
        def _():
            lane = lax.broadcasted_iota(jnp.int32, (1, lanes), 1)
            for s in range(2):
                rows = 32
                mods = [wide_ref[s, k : k + 1, :] for k in range(7)]

                @pl.loop(0, counts[s] // rows)
                def _(at):
                    cut = aligned(at, rows)
                    resid = x_ref[s][cut, :].astype(F32)
                    mean_one, inverse_one = stats(resid)
                    attn = bra[s][cut, :].astype(F32) + mods[6]
                    middle = resid + mods[2] * attn
                    mean, inverse = stats(middle)
                    normed = (middle - mean) * inverse
                    grown = dtwo[s][cut, :].astype(F32) * (1.0 + mods[4])
                    first = jnp.mean(grown, axis=-1, keepdims=True)
                    second = jnp.mean(grown * normed, axis=-1, keepdims=True)
                    d_middle = cot_ref[s][cut, :].astype(F32) + inverse * (grown - first - normed * second)
                    d_branch[s][cut, :] = (d_middle * mods[2]).astype(BF)
                    columns = (mean_one, inverse_one, mean, inverse, first, second)
                    packed = jnp.zeros((rows, lanes), F32)
                    for number, column in enumerate(columns):
                        packed = jnp.where(lane == number, column, packed)
                    stat[s][cut, :] = packed

        queries = jnp.concatenate([q_ref[0][...], q_ref[1][...]], axis=0)
        result = jnp.concatenate([o_ref[0][...], o_ref[1][...]], axis=0)
        d_attended = jnp.concatenate(
            [
                lax.dot_general(d_branch[s][...], out_ref[s], over_last, preferred_element_type=F32).astype(BF)
                for s in range(2)
            ],
            axis=0,
        )
        key_block = k_ref[...].reshape(blocks * tokens, lanes)
        value_block = v_ref[...].reshape(blocks * tokens, lanes)
        low = lax.broadcasted_iota(jnp.int32, (tokens, lanes), 1) < HD
        product = d_attended.astype(F32) * result.astype(F32)
        d_q = []
        d_k = jnp.zeros((blocks * tokens, lanes), F32)
        d_v = jnp.zeros((blocks * tokens, lanes), F32)
        for head in range(2):
            mine = low if head == 0 else jnp.logical_not(low)
            zero = jnp.zeros_like(queries)
            q_head = jnp.where(mine, queries, zero)
            d_head = jnp.where(mine, d_attended, zero)
            centre = jnp.sum(jnp.where(mine, product, 0.0), axis=-1, keepdims=True)
            log_total = lse_ref[:, head * HD : head * HD + 1]
            scores = (
                lax.dot_general(q_head, key_block, over_last, preferred_element_type=F32) * scale
            )
            weights = jnp.exp(scores - log_total)
            d_weights = lax.dot_general(d_head, value_block, over_last, preferred_element_type=F32)
            d_scores = (weights * (d_weights - centre)).astype(BF)
            d_v = d_v + lax.dot_general(
                weights.astype(BF), d_head, over_first, preferred_element_type=F32
            )
            d_k = d_k + lax.dot_general(d_scores, q_head, over_first, preferred_element_type=F32)
            d_q.append(jnp.dot(d_scores, key_block, preferred_element_type=F32))
        d_queries = (jnp.where(low, d_q[0], d_q[1]) * scale).astype(BF)
        dq[0][...] = d_queries[:img]
        dq[1][...] = d_queries[img:]
        dk_ref[...] = (d_k * scale).astype(BF).reshape(blocks, tokens, lanes)
        dv_ref[...] = d_v.astype(BF).reshape(blocks, tokens, lanes)

    heads = [pl.BlockSpec((None, c, lanes), lambda s, h: (s, 0, h)) for c in counts]
    rows = [pl.BlockSpec((None, c, full), lambda s, h: (s, 0, 0)) for c in counts]
    columns = [pl.BlockSpec((None, c, lanes), lambda s, h: (s, 0, 0)) for c in counts]
    sums = pl.BlockSpec((blocks, None, tokens, lanes), lambda s, h: (0, s, 0, h))
    return pl.pallas_call(
        kernel,
        name="attend_back",
        grid=(seqs, pairs),
        in_specs=heads * 2
        + rows * 4
        + [
            pl.BlockSpec((blocks, None, None, tokens, lanes), lambda s, h: (0, 0, s, 0, h)),
            pl.BlockSpec((blocks, None, None, tokens, lanes), lambda s, h: (0, 1, s, 0, h)),
            pl.BlockSpec((None, None, tokens, lanes), lambda s, h: (s, h, 0, 0)),
            pl.BlockSpec((2, None, 8, full), lambda s, h: (0, s, 0, 0)),
            pl.BlockSpec((2, lanes, full), lambda s, h: (0, h, 0)),
        ],
        out_specs=heads + rows + columns + [sums, sums],
        out_shape=[struct(a.shape, BF) for a in q]
        + [struct(a.shape, BF) for a in x_full]
        + [struct((seqs, c, lanes), F32) for c in counts]
        + [struct((blocks, seqs, tokens, width), BF)] * 2,
        compiler_params=pltpu.CompilerParams(vmem_limit_bytes=VMEM_LIMIT),
    )(*q, *attended, *x_full, *cot_full, *branch, *d_two, keys, keys, lse, wide, out_full)


def outer_sums(cond_rows, every, seqs):
    terms, depth = cond_rows.shape
    pods, _, width = every.shape
    kinds = 6
    room = -(-3 * terms // 16) * 16

    def kernel(cond_ref, every_ref, out_ref):
        first = pl.program_id(0) * (seqs * kinds)
        for kind in range(kinds):
            value = jnp.concatenate(
                [every_ref[p, pl.ds(first + q * kinds + kind, 1), :] for p in range(pods) for q in range(seqs)], axis=0
            )
            high = value.astype(BF).astype(F32)
            mid = (value - high).astype(BF).astype(F32)
            low = (value - high - mid).astype(BF).astype(F32)
            blank = [jnp.zeros((room - 3 * terms, width), F32)] if room > 3 * terms else []
            right = jnp.concatenate([high, mid, low] + blank, axis=0).astype(BF)
            out_ref[kind] = lax.dot_general(cond_ref[...], right, OVER_FIRST, preferred_element_type=F32)

    left = jnp.pad(jnp.concatenate([cond_rows] * 3, axis=0), ((0, room - 3 * terms), (0, 0))).astype(BF)
    return pl.pallas_call(
        kernel,
        name="outer_sums",
        grid=(2,),
        in_specs=[
            pl.BlockSpec(left.shape, lambda z: (0, 0)),
            pl.BlockSpec(every.shape, lambda z: (0, 0, 0)),
        ],
        out_specs=pl.BlockSpec((None, kinds, depth, width), lambda z: (z, 0, 0, 0)),
        out_shape=struct((2, kinds, depth, width), F32),
        compiler_params=pltpu.CompilerParams(vmem_limit_bytes=VMEM_LIMIT),
    )(left, every)


OVER_FIRST = (((0,), (0,)), ((), ()))
OVER_LAST = (((1,), (1,)), ((), ()))


def chunk_rows(img, txt, size):
    spans = [(1, 0, txt)]
    for first in range(0, img, size):
        spans.append((0, first, min(size, img - first)))
    return spans


def line_buffers(spans, slots, width):
    bufs = []
    for _, _, size in spans:
        bufs += [pltpu.VMEM((2, slots, size, width), BF)] * 2
    return bufs


def line_reduces(spans, parts, cols, place, width, bufs, ss, rs):
    reduces = []
    for number, (which, first, size) in enumerate(spans):
        src = parts[which]

        def load(block, src=src, first=first, size=size):
            return src[pl.ds(first, size), aligned(block, width)]

        reduces.append(
            LineReduce(load, cols, place, bufs[2 * number], bufs[2 * number + 1], ss.at[number], rs.at[number])
        )
    return reduces


def line_gathers(spans, outs, cols, place, width, ss, rs):
    gathers = []
    for number, (which, first, size) in enumerate(spans):
        dst = outs[which]

        def at(block, dst=dst, first=first, size=size):
            return dst.at[pl.ds(first, size), aligned(block, width)]

        gathers.append(LineGather(at, cols, place, ss.at[number], rs.at[number]))
    return gathers


class LineSum:
    def __init__(self, spans, parts, outs, cols, place, width, bufs, sems):
        self.spans, self.outs, self.place, self.width = spans, outs, place, width
        self.slots = cols - 1
        self.reduces = line_reduces(spans, parts, cols, place, width, bufs, sems[0], sems[1])
        self.gathers = line_gathers(spans, outs, cols, place, width, sems[2], sems[3])
        self.turns = len(spans) + 2 * self.slots

    def advance(self, number, step):
        which, first, size = self.spans[number]
        dst = self.outs[which]
        slots = self.slots
        if step < slots:
            self.reduces[number].step(step)
        elif step == slots:

            def store(value):
                dst[pl.ds(first, size), aligned(self.place, self.width)] = value.astype(BF)

            self.reduces[number].total(store)
            self.gathers[number].start(0)
        elif step < 2 * slots:
            self.gathers[number].arrive(step - slots - 1)
            self.gathers[number].start(step - slots)
        else:
            self.gathers[number].arrive(slots - 1)

    def turn(self, turn):
        for number in range(len(self.spans)):
            step = turn - number
            if 0 <= step <= 2 * self.slots:
                self.advance(number, step)

    def finish(self):
        for number in range(len(self.spans)):
            self.reduces[number].finish()
            self.gathers[number].finish()


def sum_branch(cols, part_img, part_txt, w_up, w_down):
    img, full = part_img.shape
    txt = part_txt.shape[0]
    width = full // cols
    spans = chunk_rows(img, txt, img // 4)
    count = len(spans)
    slots = cols - 1
    kinds, streams = ("up", "down"), ((1,), (0, 1))
    weights = (w_up, w_down)
    full_shapes = [(len(z),) + gathered_shape(k, w.shape)[1:] for k, z, w in zip(kinds, streams, weights)]
    subs = 2

    def kernel(*refs):
        parts, refs = refs[:2], refs[2:]
        shards, refs = refs[:2], refs[2:]
        outs, refs = refs[:2], refs[2:]
        fulls, refs = refs[:2], refs[2:]
        stages, refs = refs[:2], refs[2:]
        bufs, refs = refs[: 2 * count], refs[2 * count :]
        sems, (local_in, local_out, ws, wr) = refs[:4], refs[4:]
        place = lax.axis_index("col")
        line = LineSum(spans, parts, outs, cols, place, width, bufs, sems)
        flow = WeightFlow(kinds, streams, shards, fulls, subs, ws, wr)
        owns = [
            OwnCopy(
                shards[n].at[pl.ds(streams[n][0], len(streams[n]))],
                stages[n],
                flow.own_view(n),
                local_in.at[n],
                local_out.at[n],
            )
            for n in range(2)
        ]
        for own in owns:
            own.begin()
        greet(others("row", 4) + others("col", cols) + [("dp", flow.mate)])
        flow.start(1)
        line.turn(0)
        flow.start(0)
        for own in owns:
            own.settle()
        pieces = len(flow.pieces)
        y_turn = [1 + (4 * piece) // 3 for piece in range(pieces)]
        for turn in range(1, line.turns):
            line.turn(turn)
            for piece in range(pieces):
                if y_turn[piece] == turn:
                    flow.relay_y(piece)
                if y_turn[piece] + 2 == turn:
                    flow.relay_x(piece)
        for piece in range(pieces):
            if y_turn[piece] >= line.turns:
                flow.relay_y(piece)
        for piece in range(pieces):
            if y_turn[piece] + 2 >= line.turns:
                flow.relay_x(piece)
        flow.finish()
        line.finish()
        for own in owns:
            own.finish()

    return communicate(
        kernel,
        2,
        out_shape=[struct(part_img.shape, BF), struct(part_txt.shape, BF)]
        + [struct(shape, BF) for shape in full_shapes],
        in_specs=[VM, VM, ANY, ANY],
        out_specs=[VM, VM, ANY, ANY],
        scratch_shapes=[pltpu.VMEM((len(z),) + w.shape[1:], BF) for z, w in zip(streams, weights)]
        + line_buffers(spans, slots, width)
        + [pltpu.SemaphoreType.DMA((count, 2, slots))] * 4
        + [pltpu.SemaphoreType.DMA((2,))] * 2
        + [pltpu.SemaphoreType.DMA(WeightFlow.sem_shape(streams, subs))] * 2,
    )(part_img, part_txt, *weights)


class Sibling:
    def __init__(self, pairs, ss, rs):
        self.pairs, self.ss, self.rs = pairs, ss, rs

    def copy(self, number):
        src, dst = self.pairs[number]
        return send(src, dst, self.ss.at[number], self.rs.at[number], "row", flip(lax.axis_index("row")))

    def start(self):
        for number in range(len(self.pairs)):
            self.copy(number).start()

    def land(self, *numbers):
        for number in numbers:
            self.copy(number).wait_recv()

    def finish(self):
        for number in range(len(self.pairs)):
            self.copy(number).wait_send()


def row_parts(ref, buf, core):
    size = ref.shape[1] // 4
    return [(ref.at[:, aligned(2 * y + core, size)], buf.at[y]) for y in range(2)]


def token_product(left_own, left_sib, right_own, right_sib):
    return lax.dot_general(left_own, right_own, OVER_FIRST, preferred_element_type=F32) + lax.dot_general(
        left_sib, right_sib, OVER_FIRST, preferred_element_type=F32
    )


class GradFlow:
    def __init__(self, pods, product, outs, far_out, far_in, pod_out, pod_in, ys, yr, xs, xr):
        self.pods, self.product, self.outs = pods, product, outs
        self.far_out, self.far_in, self.pod_out, self.pod_in = far_out, far_in, pod_out, pod_in
        self.ys, self.yr, self.xs, self.xr = ys, yr, xs, xr
        row = lax.axis_index("row")
        self.y_of, self.far = row // 2, flip_far(row)

    @staticmethod
    def rounds(pods):
        return pods.bit_length() - 1

    @staticmethod
    def scratch(pods, count, shape):
        rounds = GradFlow.rounds(pods)
        return (
            [pltpu.VMEM((count,) + shape, BF)] * 2
            + [pltpu.VMEM((count, rounds) + shape, BF)] * 2
            + [pltpu.SemaphoreType.DMA((count,))] * 2
            + [pltpu.SemaphoreType.DMA((count, rounds))] * 2
        )

    def across(self, piece):
        return send(
            self.far_out.at[piece], self.far_in.at[piece], self.ys.at[piece], self.yr.at[piece], "row", self.far
        )

    def over(self, piece, turn):
        pod = lax.axis_index("dp")
        step = 2**turn
        peer = pod + step - 2 * step * lax.rem(pod // step, 2)
        return send(
            self.pod_out.at[piece, turn],
            self.pod_in.at[piece, turn],
            self.xs.at[piece, turn],
            self.xr.at[piece, turn],
            "dp",
            peer,
        )

    def to_far(self, piece):
        self.far_out[piece] = self.product(piece, 1 - self.y_of).astype(BF)
        self.across(piece).start()

    def here(self, piece):
        self.outs(piece)[...] = self.product(piece, self.y_of)

    def to_pod(self, piece):
        self.across(piece).wait_recv()
        self.pod_out[piece, 0] = (self.outs(piece)[...] + self.far_in[piece].astype(F32)).astype(BF)
        self.over(piece, 0).start()

    def done(self, piece):
        rounds = self.rounds(self.pods)
        for turn in range(rounds):
            self.over(piece, turn).wait_recv()
            total = self.pod_out[piece, turn].astype(F32) + self.pod_in[piece, turn].astype(F32)
            if turn == rounds - 1:
                self.outs(piece)[...] = total
            else:
                self.pod_out[piece, turn + 1] = total.astype(BF)
                self.over(piece, turn + 1).start()

    def finish(self, piece):
        self.across(piece).wait_send()
        for turn in range(self.rounds(self.pods)):
            self.over(piece, turn).wait_send()

    @staticmethod
    def friends(pods):
        pod = lax.axis_index("dp")
        found = []
        for turn in range(GradFlow.rounds(pods)):
            step = 2**turn
            found.append(("dp", pod + step - 2 * step * lax.rem(pod // step, 2)))
        return found


def sum_hidden(pods, cols, back, hidden, d_pre, act, d_mlp, first_hidden, attended):
    img, full = back[0].shape
    txt = back[1].shape[0]
    tokens = (img, txt)
    width = full // cols
    units = d_pre[0].shape[1]
    block = full // 4
    spans = chunk_rows(img, txt, img // 4)
    count = len(spans)
    slots = cols - 1
    tile = 512 if units % 512 == 0 else units

    def kernel(*refs):
        parts, hid, pre, acts, mlp, one, att = (refs[2 * n : 2 * n + 2] for n in range(7))
        refs = refs[14:]
        outs, refs = refs[:2], refs[2:]
        up_own, up_far, grad_down = refs[:3]
        one_sib, att_sib = refs[3:5], refs[5:7]
        refs = refs[7:]
        hid_sib, pre_sib, act_sib, mlp_sib = (refs[2 * n : 2 * n + 2] for n in range(4))
        refs = refs[8:]
        grad_scratch, refs = refs[:8], refs[8:]
        bufs, refs = refs[: 2 * count], refs[2 * count :]
        sems, (ss, rs) = refs[:4], refs[4:]
        place = lax.axis_index("col")
        row = lax.axis_index("row")
        core, y_of = lax.rem(row, 2), row // 2
        other = 1 - core
        line = LineSum(spans, parts, outs, cols, place, width, bufs, sems)
        pairs = []
        for s in (1, 0):
            pairs += [(acts[s], act_sib[s])] + row_parts(mlp[s], mlp_sib[s], other)
        for s in (1, 0):
            pairs += [(pre[s], pre_sib[s])] + row_parts(hid[s], hid_sib[s], other)
        for s in (1, 0):
            pairs += [(att[s], att_sib[s])] + row_parts(one[s], one_sib[s], other)
        sibling = Sibling(pairs, ss, rs)

        def down(piece, y):
            s = 1 - piece // 4
            cut = pl.ds((piece % 4) * (units // 4), units // 4)
            return token_product(
                acts[s][:, cut], act_sib[s][:, cut], mlp[s][:, aligned(2 * y + core, block)], mlp_sib[s][y]
            )

        def down_view(piece):
            return grad_down.at[1 - piece // 4, pl.ds((piece % 4) * (units // 4), units // 4), :]

        grads = GradFlow(pods, down, down_view, *grad_scratch)
        greet(others("row", 4) + others("col", cols) + GradFlow.friends(pods))
        sibling.start()
        line.turn(0)

        def up(s, y, write):
            left_own = hid[s][:, aligned(2 * y + core, block)]
            left_sib = hid_sib[s][y]

            @pl.loop(0, units // tile)
            def _(at):
                cut = aligned(at, tile)
                write(cut, token_product(left_own, left_sib, pre[s][:, cut], pre_sib[s][:, cut]))

        def up_to_far(s):
            sibling.land(9 - 3 * s, 10 - 3 * s, 11 - 3 * s)

            def write(cut, value):
                up_far[s, :, cut] = value.astype(BF)

            up(s, 1 - y_of, write)

        def up_here(s):
            def write(cut, value):
                up_own[s, :, cut] = value

            up(s, y_of, write)

        def down_to_far(s):
            sibling.land(3 - 3 * s, 4 - 3 * s, 5 - 3 * s)
            for piece in range(4):
                grads.to_far(4 * (1 - s) + piece)

        def down_here(s):
            for piece in range(4):
                grads.here(4 * (1 - s) + piece)

        work = {
            0: lambda: down_to_far(1),
            1: lambda: down_to_far(0),
            2: lambda: down_here(1),
            3: lambda: down_here(0),
            4: lambda: grads.to_pod(0),
            5: lambda: grads.to_pod(1),
            6: lambda: grads.to_pod(2),
            7: lambda: grads.to_pod(3),
            8: lambda: (grads.to_pod(4), grads.to_pod(5)),
            10: lambda: grads.to_pod(6),
        }
        for turn in range(line.turns):
            if turn > 0:
                line.turn(turn)
            if turn in work:
                work[turn]()
        grads.to_pod(7)
        for s in (1, 0):
            up_to_far(s)
            up_here(s)
        sibling.land(*range(12, 18))
        for piece in range(8):
            grads.done(piece)
        sibling.finish()
        for piece in range(8):
            grads.finish(piece)
        line.finish()

    arrays = list(back) + list(hidden) + list(d_pre) + list(act) + list(d_mlp) + list(first_hidden) + list(attended)
    return communicate(
        kernel,
        3,
        out_shape=[struct(b.shape, BF) for b in back]
        + [
            struct((2, block, units), F32),
            struct((2, block, units), BF),
            struct((2, units, block), F32),
        ]
        + [struct((2, t, block), BF) for t in tokens]
        + [struct(a.shape, BF) for a in attended],
        in_specs=[VM] * 10 + [ANY] * 4,
        out_specs=[VM] * 5 + [ANY] * 4,
        scratch_shapes=[pltpu.VMEM((2, t, block), BF) for t in tokens]
        + [pltpu.VMEM((t, units), BF) for t in tokens]
        + [pltpu.VMEM((t, units), BF) for t in tokens]
        + [pltpu.VMEM((2, t, block), BF) for t in tokens]
        + GradFlow.scratch(pods, 8, (units // 4, block))
        + line_buffers(spans, slots, width)
        + [pltpu.SemaphoreType.DMA((count, 2, slots))] * 4
        + [pltpu.SemaphoreType.DMA((18,))] * 2,
    )(*arrays)


def sum_keys(pods, cols, d_key, d_value, part_img, part_txt, img, attended, attended_sib, d_branch):
    _, seqs, tokens, width = d_key.shape
    txt = tokens - img
    img_rows, full = part_img.shape
    block = full // 4
    spans = chunk_rows(img_rows, part_txt.shape[0], img_rows // 4)
    count = len(spans)
    slots = cols - 1
    lots = [(which, seq) for which in range(2) for seq in range(seqs)]
    lot_count = len(lots)

    def kernel(*refs):
        dk_ref, dv_ref = refs[:2]
        parts = refs[2:4]
        att, att_sib, bra = refs[4:6], refs[6:8], refs[8:10]
        kv_img, kv_txt = refs[10:12]
        line_out = refs[12:14]
        grad_ref = refs[14]
        near_in, far_out, far_in, ns, nr, fs, fr = refs[15:22]
        bra_sib = refs[22:24]
        ss, rs = refs[24:26]
        grad_scratch = refs[26:34]
        refs = refs[34:]
        bufs, refs = refs[: 2 * count], refs[2 * count :]
        rss, rsr = refs
        row = lax.axis_index("row")
        place = lax.axis_index("col")
        core = lax.rem(row, 2)
        sib, far = flip(row), flip_far(row)
        sources = (dk_ref, dv_ref)
        reduces = line_reduces(spans, parts, cols, place, width, bufs, rss, rsr)
        sibling = Sibling(
            [pair for s in range(2) for pair in row_parts(bra[s], bra_sib[s], 1 - core)], ss, rs
        )

        def product(s, y):
            return token_product(
                att[s][...], att_sib[s][...], bra[s][:, aligned(2 * y + core, block)], bra_sib[s][y]
            )

        grads = GradFlow(pods, product, lambda s: grad_ref.at[s], *grad_scratch)
        greet(others("row", 4) + others("col", cols) + GradFlow.friends(pods))

        def near(lot, number):
            which, seq = lots[lot]
            target = flip(far) if number == 0 else sib
            return send(
                sources[which].at[target, seq],
                near_in.at[lot, number],
                ns.at[lot, number],
                nr.at[lot, number],
                "row",
                sib,
            )

        def across(lot):
            return send(far_out.at[lot], far_in.at[lot], fs.at[lot], fr.at[lot], "row", far)

        for lot in range(lot_count):
            near(lot, 0).start()
        sibling.start()
        for lot in range(lot_count):
            near(lot, 1).start()

        def line_step(number, step):
            which, first, size = spans[number]
            dst = line_out[which]
            if step < slots:
                reduces[number].step(step)
            else:

                def store(value):
                    dst[pl.ds(first, size), :] = value

                reduces[number].total(store)

        def near_step(lot):
            which, seq = lots[lot]
            near(lot, 0).wait_recv()
            far_out[lot] = (sources[which][far, seq].astype(F32) + near_in[lot, 0].astype(F32)).astype(BF)
            across(lot).start()

        def far_step(lot):
            which, seq = lots[lot]
            near(lot, 1).wait_recv()
            across(lot).wait_recv()
            total = (
                sources[which][row, seq].astype(F32)
                + near_in[lot, 1].astype(F32)
                + far_in[lot].astype(F32)
            ).astype(BF)
            kv_img[which, seq] = total[:img]
            kv_txt[which, seq] = total[img:]

        for number in range(count):
            line_step(number, 0)
        for lot in range(lot_count):
            near_step(lot)
        sibling.land(0, 1, 2, 3)
        for s in range(2):
            grads.to_far(s)
        for turn in range(1, slots):
            for number in range(count):
                line_step(number, turn)
            if turn == 1:
                for s in range(2):
                    grads.here(s)
            far_step(turn - 1)
        for lot in range(slots - 1, lot_count):
            far_step(lot)
        for s in range(2):
            grads.to_pod(s)
        for number in range(count):
            line_step(number, slots)
        for s in range(2):
            grads.done(s)
        sibling.finish()
        for lot in range(lot_count):
            for number in range(2):
                near(lot, number).wait_send()
            across(lot).wait_send()
        for number in range(count):
            reduces[number].finish()
        for s in range(2):
            grads.finish(s)

    return communicate(
        kernel,
        4,
        out_shape=[
            struct((2, seqs, img, width), BF),
            struct((2, seqs, txt, width), BF),
            struct((img_rows, width), F32),
            struct((part_txt.shape[0], width), F32),
            struct((2, width, block), F32),
        ],
        in_specs=[VM] * 10,
        out_specs=[VM] * 5,
        scratch_shapes=[
            pltpu.VMEM((lot_count, 2, tokens, width), BF),
            pltpu.VMEM((lot_count, tokens, width), BF),
            pltpu.VMEM((lot_count, tokens, width), BF),
            pltpu.SemaphoreType.DMA((lot_count, 2)),
            pltpu.SemaphoreType.DMA((lot_count, 2)),
            pltpu.SemaphoreType.DMA((lot_count,)),
            pltpu.SemaphoreType.DMA((lot_count,)),
        ]
        + [pltpu.VMEM((2, b.shape[0], block), BF) for b in d_branch]
        + [pltpu.SemaphoreType.DMA((4,))] * 2
        + GradFlow.scratch(pods, 2, (width, block))
        + line_buffers(spans, slots, width)
        + [pltpu.SemaphoreType.DMA((count, 2, slots))] * 2,
    )(d_key, d_value, part_img, part_txt, *attended, *attended_sib, *d_branch)


def sum_last(
    pods, cols, d_q, d_kv, qkv, hidden, hidden_sib, xs, cots, branch, d_two, mlp, stat_cols, tables, b_down, up_rows, slope, ada
):
    seqs = tables.shape[2]
    tokens = [x.shape[0] for x in xs]
    counts = [t // seqs for t in tokens]
    width = xs[0].shape[1]
    full = width * cols
    block = full // 4
    spans = chunk_rows(tokens[0], tokens[1], tokens[0] // 4)
    count = len(spans)
    slots = cols - 1
    pieces = [(s, k) for s in (1, 0) for k in range(3)]
    lanes = tokens[0] + 128
    firsts = (0, tokens[0])
    mods_rows = 2 * seqs * 6
    up_count = up_rows.shape[0]
    pack_rows = mods_rows + 8 + up_count

    def kernel(*refs):
        takes = iter(refs)

        def two():
            return (next(takes), next(takes))

        dq, dkv = two(), two()
        qkv_any = next(takes)
        hid, hid_sib, x_ref, cot_ref, bra_any, dtwo_any, mlp_ref, stat = (two() for _ in range(8))
        table_ref, down_ref, up_ref, slope_ref, ada_any = (next(takes) for _ in range(5))
        out_ref, dx_ref = two(), two()
        grad_ref, every_ref, rest_ref, mods_sum, silu_ref = (next(takes) for _ in range(5))
        dq_sib, dkv_sib, parts, d_one, grown = (two() for _ in range(5))
        sums_mine, sums_in, pack_mine, pack_in, silu_mine, silu_in = (next(takes) for _ in range(6))
        ss, rs, ms, mr, ps, pr, es, er, cs, cr = (next(takes) for _ in range(10))
        grad_scratch = [next(takes) for _ in range(8)]
        bufs = [next(takes) for _ in range(2 * count)]
        rss, rsr = next(takes), next(takes)
        qkv_ref, ada_ref = next(takes), next(takes)
        bra, dtwo = two(), two()
        loads = next(takes)
        row = lax.axis_index("row")
        place = lax.axis_index("col")
        pod = lax.axis_index("dp")
        core = lax.rem(row, 2)
        mine = aligned(place, width)
        w_loads = [
            pltpu.make_async_copy(qkv_any.at[s, k], qkv_ref.at[s, k], loads.at[3 * s + k])
            for s in (1, 0)
            for k in range(3)
        ]
        late_loads = [pltpu.make_async_copy(ada_any, ada_ref, loads.at[6])]
        for s in range(2):
            late_loads.append(pltpu.make_async_copy(bra_any[s].at[:, mine], bra[s], loads.at[7 + s]))
            late_loads.append(pltpu.make_async_copy(dtwo_any[s].at[:, mine], dtwo[s], loads.at[9 + s]))
        for load in w_loads + late_loads:
            load.start()
        reduces = line_reduces(spans, parts, cols, place, width, bufs, rss, rsr)
        sibling = Sibling([pair for s in (1, 0) for pair in ((dq[s], dq_sib[s]), (dkv[s], dkv_sib[s]))], ss, rs)

        def projected(own, s, k):
            return own[0][s][...] if k == 0 else own[1][s][k - 1]

        def product(piece, y):
            s, k = pieces[piece]
            return token_product(
                hid[s][:, aligned(2 * y + core, block)],
                hid_sib[s][y],
                projected((dq, dkv), s, k),
                projected((dq_sib, dkv_sib), s, k),
            )

        def out_view(piece):
            s, k = pieces[piece]
            return grad_ref.at[s, k]

        grads = GradFlow(pods, product, out_view, *grad_scratch)
        greet(others("col", cols) + others("row", 4) + others("dp", pods))
        sibling.start()
        sibling.land(0, 1)
        for k in range(3):
            grads.to_far(k)
        for number, (s, first, size) in enumerate(spans):
            rows = pl.ds(first, size)
            if first == 0:
                for k in range(3):
                    w_loads[3 * (1 - s) + k].wait()
            term = lax.dot_general(dq[s][rows, :], qkv_ref[s, 0], OVER_LAST, preferred_element_type=F32)
            for k in range(2):
                term = term + lax.dot_general(
                    dkv[s][k, rows, :], qkv_ref[s, k + 1], OVER_LAST, preferred_element_type=F32
                )
            parts[s][rows, :] = term.astype(BF)
            reduces[number].step(0)
        sibling.land(2, 3)
        for k in range(3):
            grads.to_far(3 + k)
        for number in range(count):
            reduces[number].step(1)
        for piece in range(6):
            grads.here(piece)
        for load in late_loads:
            load.wait()

        def segment(s, q):
            return pl.ds(q * counts[s], counts[s])

        def modulation(s, q, position):
            return table_ref[place, s, q, pl.ds(position, 1), :]

        def put(index, value):
            pack_mine[pl.ds(index, 1), :] = value

        def over_tokens(value):
            return jnp.sum(value, axis=0, keepdims=True)

        def early(s):
            d_out = d_down = None
            for q in range(seqs):
                rows = segment(s, q)
                at = (s * seqs + q) * 6
                column = stat[s][rows, :]
                cot = cot_ref[s][rows, :].astype(F32)
                d_hidden = dtwo[s][rows, :].astype(F32)
                attn = bra[s][rows, :].astype(F32) + modulation(s, q, 6)
                gate_a, gate_m = modulation(s, q, 2), modulation(s, q, 5)
                middle = x_ref[s][rows, :].astype(F32) + gate_a * attn
                mlp_branch = mlp_ref[s][rows, :] + down_ref[pl.ds(s, 1), :]
                out_ref[s][rows, :] = (middle + gate_m * mlp_branch).astype(BF)
                normed = (middle - column[:, 2:3]) * column[:, 3:4]
                d_normed = d_hidden * (1.0 + modulation(s, q, 4))
                d_middle = cot + column[:, 3:4] * (d_normed - column[:, 4:5] - normed * column[:, 5:6])
                dx_ref[s][rows, :] = d_middle
                put(at + 2, over_tokens(d_middle * attn))
                put(at + 3, over_tokens(d_hidden))
                put(at + 4, over_tokens(d_hidden * normed))
                put(at + 5, over_tokens(cot * mlp_branch))
                first, second = over_tokens(d_middle * gate_a), over_tokens(cot * gate_m)
                d_out = first if d_out is None else d_out + first
                d_down = second if d_down is None else d_down + second
            put(mods_rows + 4 + s, d_out)
            put(mods_rows + 6 + s, d_down)
            put(mods_rows + 2 * s, over_tokens(dq[s][...].astype(F32)))
            put(mods_rows + 2 * s + 1, over_tokens(dkv[s][1].astype(F32)))

        pack_mine[pl.ds(mods_rows + 8, up_count), :] = up_ref[...]
        early(1)
        for number in range(count):
            for turn in range(2, slots):
                reduces[number].step(turn)
        early(0)
        grads.to_pod(0)
        grads.to_pod(1)
        for number, (s, first, size) in enumerate(spans):

            def store(value, s=s, first=first, size=size):
                d_one[s][pl.ds(first, size), :] = value

            reduces[number].total(store)

        one_row = lax.broadcasted_iota(jnp.int32, (8, width), 0)
        pick = [jnp.where(one_row == k, 1.0, 0.0).astype(F32) for k in range(2)]
        for s in range(2):
            for q in range(seqs):
                rows = segment(s, q)
                at = (s * seqs + q) * 6
                column = stat[s][rows, :]
                normed = (x_ref[s][rows, :].astype(F32) - column[:, 0:1]) * column[:, 1:2]
                d_hidden = d_one[s][rows, :]
                put(at, over_tokens(d_hidden))
                put(at + 1, over_tokens(d_hidden * normed))
                value = d_hidden * (1.0 + modulation(s, q, 1))
                d_one[s][rows, :] = value
                grown[s][rows, :] = value * normed
            exact = lax.Precision.HIGHEST
            sums_mine[:, pl.ds(firsts[s], tokens[s])] = lax.dot_general(
                pick[0], d_one[s][...], OVER_LAST, precision=exact, preferred_element_type=F32
            ) + lax.dot_general(pick[1], grown[s][...], OVER_LAST, precision=exact, preferred_element_type=F32)

        def small(step):
            return send(
                sums_mine, sums_in.at[step - 1], ms.at[step - 1], mr.at[step - 1], "col", lax.rem(place + step, cols)
            )

        for step in range(1, cols):
            small(step).start()

        def pack_copy(step):
            return send(
                pack_mine, pack_in.at[step - 1], ps.at[step - 1], pr.at[step - 1], "row", lax.rem(row + step, 4)
            )

        for step in range(1, 4):
            pack_copy(step).start()
        grads.to_pod(2)
        total = sums_mine[...]
        for step in range(1, cols):
            small(step).wait()
            total = total + sums_in[step - 1]
        lane = lax.broadcasted_iota(jnp.int32, (8, 128), 1)
        sublane = lax.broadcasted_iota(jnp.int32, (8, 128), 0)
        spread = jnp.where(sublane == lane // HD, 1.0 / full, 0.0).astype(F32)
        for s in range(2):
            means = lax.dot_general(
                total[:, firsts[s] : firsts[s] + tokens[s]],
                spread,
                OVER_FIRST,
                precision=lax.Precision.HIGHEST,
                preferred_element_type=F32,
            )
            column = stat[s][...]
            normed = (x_ref[s][...].astype(F32) - column[:, 0:1]) * column[:, 1:2]
            dx_ref[s][...] = dx_ref[s][...] + column[:, 1:2] * (
                d_one[s][...] - means[:, 0:1] - normed * means[:, HD : HD + 1]
            )
        grads.to_pod(3)

        def ordered(own, theirs, index, size):
            value = jnp.zeros_like(own)
            for number in range(size):
                gap = lax.rem(index - number + size, size)
                value = value + jnp.where(gap == 0, own, theirs[jnp.maximum(gap - 1, 0)])
            return value

        for step in range(1, 4):
            pack_copy(step).wait()
        packed = ordered(pack_mine[...], pack_in, row, 4)
        every_ref[pod] = packed

        def every_copy(step):
            at = every_ref.at[pod]
            return send(at, at, es.at[step - 1], er.at[step - 1], "dp", lax.rem(pod + step, pods))

        for step in range(1, pods):
            every_copy(step).start()
        d_silu = jnp.zeros((8, width), F32)
        for s in range(2):
            for k in range(6):
                rows = [packed[(s * seqs + q) * 6 + k : (s * seqs + q) * 6 + k + 1] for q in range(seqs)]
                value = jnp.concatenate(rows, axis=0)
                high = value.astype(BF)
                rest = value - high.astype(F32)
                mid = rest.astype(BF)
                low = (rest - mid.astype(F32)).astype(BF)
                terms = jnp.concatenate(
                    [high.astype(F32), mid.astype(F32), low.astype(F32), jnp.zeros((8 - 3 * seqs, width), F32)], axis=0
                ).astype(BF)
                d_silu = d_silu + lax.dot_general(terms, ada_ref[s, k], OVER_LAST, preferred_element_type=F32)
        silu_mine[...] = d_silu[:seqs] + d_silu[seqs : 2 * seqs] + d_silu[2 * seqs : 3 * seqs]

        def silu_copy(step):
            return send(
                silu_mine, silu_in.at[step - 1], cs.at[step - 1], cr.at[step - 1], "col", lax.rem(place + step, cols)
            )

        for step in range(1, cols):
            silu_copy(step).start()
        for piece in (4, 5):
            grads.to_pod(piece)
        for step in range(1, cols):
            silu_copy(step).wait()
        silu_ref[...] = ordered(silu_mine[...], silu_in, place, cols) * slope_ref[...]
        for piece in range(6):
            grads.done(piece)
        for step in range(1, pods):
            source = lax.rem(pod - step + pods, pods)
            at = every_ref.at[source]
            send(at, at, es.at[step - 1], er.at[step - 1], "dp", source).wait_recv()
            every_copy(step).wait_send()
        rest_ref[...] = sum(every_ref[p, pl.ds(mods_rows, 8 + up_count), :] for p in range(pods))
        for s in range(2):
            mods_sum[pl.ds(6 * s, 6), :] = sum(
                every_ref[p, pl.ds((s * seqs + q) * 6, 6), :] for p in range(pods) for q in range(seqs)
            )
        sibling.finish()
        for number in range(count):
            reduces[number].finish()
        for piece in range(6):
            grads.finish(piece)

    arrays = (
        list(d_q)
        + list(d_kv)
        + [qkv]
        + list(hidden)
        + list(hidden_sib)
        + list(xs)
        + list(cots)
        + list(branch)
        + list(d_two)
        + list(mlp)
        + list(stat_cols)
        + [tables, b_down, up_rows, slope, ada]
    )
    dma = pltpu.SemaphoreType.DMA
    return communicate(
        kernel,
        5,
        out_shape=[struct((t, width), BF) for t in tokens]
        + [struct((t, width), F32) for t in tokens]
        + [
            struct((2, 3, block, width), F32),
            struct((pods, pack_rows, width), F32),
            struct((8 + up_count, width), F32),
            struct((12, width), F32),
            struct((seqs, width), F32),
        ],
        in_specs=[VM] * 4 + [ANY] + [VM] * 8 + [ANY] * 4 + [VM] * 8 + [ANY],
        out_specs=[VM] * 9,
        scratch_shapes=[pltpu.VMEM(a.shape, BF) for a in d_q]
        + [pltpu.VMEM(a.shape, BF) for a in d_kv]
        + [pltpu.VMEM((t, full), BF) for t in tokens]
        + [pltpu.VMEM((t, width), F32) for t in tokens] * 2
        + [
            pltpu.VMEM((8, lanes), F32),
            pltpu.VMEM((slots, 8, lanes), F32),
            pltpu.VMEM((pack_rows, width), F32),
            pltpu.VMEM((3, pack_rows, width), F32),
            pltpu.VMEM((seqs, width), F32),
            pltpu.VMEM((slots, seqs, width), F32),
        ]
        + [dma((4,))] * 2
        + [dma((slots,))] * 2
        + [dma((3,))] * 2
        + [dma((pods - 1,))] * 2
        + [dma((slots,))] * 2
        + GradFlow.scratch(pods, 6, (block, width))
        + line_buffers(spans, slots, width)
        + [dma((count, 2, slots))] * 2
        + [pltpu.VMEM(qkv.shape, BF), pltpu.VMEM(ada.shape, BF)]
        + [pltpu.VMEM((t, width), BF) for t in tokens] * 2
        + [dma((11,))],
    )(*arrays)


def gelu_pair(inputs):
    inner = GELU_ROOT * (inputs + GELU_CUBIC * inputs * inputs * inputs)
    tanh_value = jnp.tanh(inner)
    result = 0.5 * inputs * (1.0 + tanh_value)
    derivative = 0.5 * (1.0 + tanh_value) + 0.5 * inputs * (
        1.0 - tanh_value * tanh_value
    ) * GELU_ROOT * (1.0 + 3.0 * GELU_CUBIC * inputs * inputs)
    return (result, derivative)


def stats(values):
    mean = jnp.mean(values, axis=-1, keepdims=True)
    centred = values - mean
    inverse = lax.rsqrt(jnp.mean(centred * centred, axis=-1, keepdims=True) + EPSILON)
    return mean, inverse


def dot_f32(left, right):
    return jnp.einsum("td,de->te", left, right, preferred_element_type=F32)


def dot_back(left, right):
    return jnp.einsum("te,de->td", left, right, preferred_element_type=F32)


def local(
    dp_count,
    row_count,
    col_count,
    x_img,
    x_txt,
    condition,
    w_qkv,
    b_qv,
    w_out,
    b_out,
    w_up,
    b_up,
    w_down,
    b_down,
    w_ada,
    b_ada,
    cot_img,
    cot_txt,
):
    seqs, img, width = x_img.shape
    txt = x_txt.shape[1]
    full = width * col_count
    counts = (img, txt)

    cond_wide = condition.astype(F32)
    cond_act = jax.nn.silu(cond_wide).astype(BF)
    sigmoid_cond = jax.nn.sigmoid(cond_wide)
    ada = jnp.transpose(w_ada, (0, 2, 1, 3))
    table = jnp.einsum("sc,zkcd->zskd", cond_act, ada, preferred_element_type=F32)
    table = jnp.pad(table, ((0, 0), (0, 0), (0, 2), (0, 0)))
    bias_six = jnp.broadcast_to(b_ada[:, None], (2, seqs, 6, width))
    bias_rest = jnp.broadcast_to(b_out[:, None, None], (2, seqs, 2, width))
    *x_full, qkv_full, out_full, tables, all_cond = prologue(
        dp_count,
        col_count,
        x_img,
        x_txt,
        jnp.transpose(w_qkv, (0, 2, 1, 3)),
        w_out,
        table,
        jnp.concatenate([bias_six, bias_rest], axis=2),
        jnp.pad(cond_act.astype(F32), ((0, 8 - seqs), (0, 0))),
    )
    wide = jnp.transpose(tables, (1, 2, 3, 0, 4)).reshape(2, seqs, 8, full)

    def mod(stream, position):
        return wide[stream, :, position][:, None, :]

    flat = [a.reshape(seqs * counts[s], full) for s, a in enumerate(x_full)]
    *front_out, cot_one, cot_two, up_one = front(
        col_count, flat, wide, qkv_full, b_qv, (cot_img, cot_txt), w_up
    )
    cot_full = [cot_one, cot_two]
    hidden_one, queries, keys = front_out[:2], front_out[2:4], front_out[4]
    attended, lse = front_out[5:7], front_out[7]
    resid = [array.astype(F32) for array in x_full]
    out_terms = [dot_f32(attended[s], out_full[s]).astype(BF) for s in range(2)]
    *branch_sum, up_two, down_full = sum_branch(col_count, out_terms[0], out_terms[1], w_up, w_down)
    up_full = [up_one[0], up_two[0]]
    attn_branch = [
        branch_sum[s].reshape(seqs, counts[s], full).astype(F32) + mod(s, 6) for s in range(2)
    ]
    middle = [resid[s] + mod(s, 2) * attn_branch[s] for s in range(2)]
    stats_two = [stats(array) for array in middle]
    normed_two = [(middle[s] - stats_two[s][0]) * stats_two[s][1] for s in range(2)]
    hidden_two = [
        (normed_two[s] * (1.0 + mod(s, 4)) + mod(s, 3)).astype(BF).reshape(seqs * counts[s], full)
        for s in range(2)
    ]
    d_mlp_bf = [
        (cot_full[s].astype(F32) * mod(s, 5)).astype(BF).reshape(seqs * counts[s], full)
        for s in range(2)
    ]
    act, d_pre, d_pre_bf, down_terms, up_back = [], [], [], [], []
    for s in range(2):
        pre = dot_f32(hidden_two[s], up_full[s]) + b_up[s]
        value, slope = gelu_pair(pre)
        act.append(value.astype(BF))
        d_pre.append(dot_back(d_mlp_bf[s], down_full[s]) * slope)
        d_pre_bf.append(d_pre[s].astype(BF))
        up_back.append(dot_back(d_pre_bf[s], up_full[s]).astype(BF))
        down_terms.append(dot_f32(act[s], down_full[s]).astype(BF))

    d_two_img, d_two_txt, up_own, up_far, grad_down, *paired = sum_hidden(
        dp_count,
        col_count, up_back, hidden_two, d_pre_bf, act, d_mlp_bf, hidden_one, attended
    )
    hidden_pairs, attended_pairs = paired[:2], paired[2:]

    far_perm = [(r, (r + 2) % 4) for r in range(row_count)]

    def pod_sum(rounded):
        step = 1
        while step < dp_count:
            perm = [(d, d ^ step) for d in range(dp_count)]
            moved = lax.ppermute(rounded, "dp", perm)
            value = rounded.astype(F32) + moved.astype(F32)
            rounded = value.astype(BF)
            step *= 2
        return value

    def up_near(own, far):
        return (own + lax.ppermute(far, "row", far_perm).astype(F32)).astype(BF)

    near_one = up_near(up_own[0], up_far[0])

    d_two = [d_two_img, d_two_txt]
    shaped = [[a.reshape(seqs, counts[s], full) for a in (branch_sum[s], d_two[s])] for s in range(2)]
    dq_img, dq_txt, *d_branch, stat_img, stat_txt, d_key, d_value = attend_back(
        [queries[s].reshape(seqs, counts[s], width) for s in range(2)],
        keys,
        [attended[s].reshape(seqs, counts[s], width) for s in range(2)],
        lse,
        x_full,
        cot_full,
        [shaped[0][0], shaped[1][0]],
        [shaped[0][1], shaped[1][1]],
        wide,
        out_full,
    )
    d_branch_bf = [d_branch[s].reshape(seqs * counts[s], full) for s in range(2)]
    stat_cols = [stat_img.reshape(seqs * img, 2 * HD), stat_txt.reshape(seqs * txt, 2 * HD)]
    d_key, d_value, near_one, down_terms, far_two = lax.optimization_barrier(
        (d_key, d_value, near_one, down_terms, up_far[1])
    )
    grad_up_one = pod_sum(near_one)
    near_two = up_near(up_own[1], far_two)
    kv_img, kv_txt, mlp_img, mlp_txt, grad_out = sum_keys(
        dp_count, col_count, d_key, d_value, *down_terms, img, attended, attended_pairs, d_branch_bf
    )

    kv_img, kv_txt, near_two = lax.optimization_barrier((kv_img, kv_txt, near_two))
    grad_up_two = pod_sum(near_two)
    grad_up = jnp.stack([grad_up_one, grad_up_two], axis=0)

    flat = [(seqs * c, width) for c in counts]
    up_rows = jnp.concatenate([jnp.sum(d_pre[s], axis=0).reshape(-1, width) for s in range(2)], axis=0)
    out_img, out_txt, dx_img, dx_txt, grad_qkv, every, rest, mods_sum, d_condition = sum_last(
        dp_count,
        col_count,
        [dq_img.reshape(flat[0]), dq_txt.reshape(flat[1])],
        [kv_img.reshape((2,) + flat[0]), kv_txt.reshape((2,) + flat[1])],
        qkv_full,
        hidden_one,
        hidden_pairs,
        [x_img.reshape(flat[0]), x_txt.reshape(flat[1])],
        [cot_img.reshape(flat[0]), cot_txt.reshape(flat[1])],
        branch_sum,
        d_two,
        [mlp_img, mlp_txt],
        stat_cols,
        tables,
        b_down,
        up_rows,
        sigmoid_cond * (1.0 + cond_wide * (1.0 - sigmoid_cond)),
        ada,
    )
    grad_qkv = jnp.transpose(grad_qkv, (0, 2, 1, 3))
    grad_bqv = rest[:4].reshape(2, 2, width)
    grad_bout = rest[4:6]
    grad_bdown = rest[6:8]
    grad_bup = rest[8:].reshape(2, -1)
    grad_ada = outer_sums(all_cond[:, :seqs].reshape(dp_count * seqs, width), every, seqs)
    grad_ada = jnp.transpose(grad_ada, (0, 2, 1, 3))
    grad_bada = mods_sum.reshape(2, 6, width)
    return (
        out_img.reshape(x_img.shape),
        out_txt.reshape(x_txt.shape),
        dx_img.reshape(x_img.shape),
        dx_txt.reshape(x_txt.shape),
        d_condition,
        grad_qkv,
        grad_bqv,
        grad_out,
        grad_bout,
        grad_up,
        grad_bup,
        grad_down,
        grad_bdown,
        grad_ada,
        grad_bada,
    )


def solution(mesh):
    placed = (
        P("dp", "row", "col"),
        P("dp", "row", "col"),
        P("dp", "row"),
        P(None, "row", None, "col"),
        P(None, None, "col"),
        P(None, "col", "row"),
        P(None, "col"),
        P(None, "row", "col"),
        P(None, "col"),
        P(None, "col", "row"),
        P(None, "col"),
        P(None, "row", None, "col"),
        P(None, None, "col"),
        P("dp", "row", "col"),
        P("dp", "row", "col"),
    )

    def body(*args):
        return local(mesh.shape["dp"], mesh.shape["row"], mesh.shape["col"], *args)

    return jax.shard_map(
        body,
        mesh=mesh,
        in_specs=placed,
        out_specs=(
            P("dp", "row", "col"),
            P("dp", "row", "col"),
            P("dp", "row", "col"),
            P("dp", "row", "col"),
            P("dp", "row"),
            P(None, "row", None, "col"),
            P(None, None, "col"),
            P(None, "col", "row"),
            P(None, "col"),
            P(None, "row", "col"),
            P(None, "col"),
            P(None, "col", "row"),
            P(None, "col"),
            P(None, "row", None, "col"),
            P(None, None, "col"),
        ),
        check_vma=False,
    )
```
